256 devices in a mesh: band: 128 (over z, y, x), chan: 2 (over core).
Axes of the slice: x: 4, y: 4, z: 8, core: 2. Of those that a mesh axis runs over, the one named last changes fastest.
Arguments:
- grid_latent: bfloat16 [147456, 512], P(('band', 'chan')), may hold values from -6 to 6
- edge_latent: bfloat16 [294912, 512], P(('band', 'chan')), may hold values from -6 to 6
- mesh_latent: bfloat16 [40960, 512], P(('band', 'chan')), may hold values from -6 to 6
- mesh_cotangent: bfloat16 [40960, 512], P(('band', 'chan')), may hold values from -6 to 6
- w_grid: bfloat16 [512, 512], P(None, 'chan'), may hold values from -0.15625 to 0.15625
- w_mesh: bfloat16 [512, 512], P(None, 'chan'), may hold values from -0.15625 to 0.15625
- w_edge: bfloat16 [512, 512], P(None, 'chan'), may hold values from -0.15625 to 0.15625
- bias: float32 [512], P('chan'), may hold values from -3 to 3
- w_out: bfloat16 [512, 512], P('chan'), may hold values from -0.25 to 0.25
- senders: int32 [294912], P('band'), may hold values from 0 to 147455, as said below
- receivers: int32 [294912], P('band'), may hold values from 0 to 40959, as said below
- edge_count: int32 [128], P('band'), may hold values from 1152 to 2304, as said below
Outputs:
- grad_grid: bfloat16 [147456, 512], P(('band', 'chan'))
- grad_edge: bfloat16 [294912, 512], P(('band', 'chan'))
- grad_mesh: bfloat16 [40960, 512], P(('band', 'chan'))
- grad_w_grid: float32 [512, 512], P(None, 'chan')
- grad_w_mesh: float32 [512, 512], P(None, 'chan')
- grad_w_edge: float32 [512, 512], P(None, 'chan')
- grad_bias: float32 [512], P('chan')
- grad_w_out: float32 [512, 512], P('chan')
The draws below stay inside these ranges and needn't reach their ends.
Inputs may be any that keep to these rules, and one draw needn't show every extreme that they name: `senders`: an edge of band j (rows j * 2304 to (j + 1) * 2304 - 1) has its sender among grid rows j * 1152 to (j + 1) * 1152 - 1. `receivers`: an edge of band j has its receiver among mesh rows of owners j - 1, j, j + 1 (owner i holds rows i * 320 to (i + 1) * 320 - 1). `edge_count`: some band uses all 2304 slots.
All inputs are finite; a program needn't handle non-finite values.
Results may differ from the reference program's by a relative error of at most 0.0059.
Values may be sent and summed in bfloat16 or wider, within the bound.
No kernel may reach another device: no remote copies, remote signals or barrier semaphores. Data moves between devices by JAX's collectives and lax.ppermute only.
A program may use at most 64 MiB of HBM per device.

```python
import jax
import jax.numpy as jnp
from jax import lax

D = 512
H = 512
E_DEV = 2304
MB = 320
G_DEV = 1152
EDGES = 294912
GRID = 147456
MESH = 40960
N_CHAN = 2


def draw_senders(key, part):
    band_of = jnp.arange(EDGES, dtype=jnp.int32) // E_DEV
    return band_of * G_DEV + jax.random.randint(key, (EDGES,), 0, G_DEV, dtype=jnp.int32)


def draw_receivers(key, part):
    first, second = jax.random.split(jax.random.fold_in(key, 11))
    band_of = jnp.arange(EDGES, dtype=jnp.int32) // E_DEV
    offset = jax.random.randint(first, (EDGES,), -1, 2, dtype=jnp.int32)
    owner = jnp.clip(band_of + offset, 0, EDGES // E_DEV - 1)
    return owner * MB + jax.random.randint(second, (EDGES,), 0, MB, dtype=jnp.int32)


def draw_edge_count(key, part):
    first, second = jax.random.split(jax.random.fold_in(key, 23))
    bands = EDGES // E_DEV
    counts = jax.random.randint(first, (bands,), E_DEV // 2, E_DEV + 1, dtype=jnp.int32)
    fullest = jax.random.randint(second, (), 0, bands, dtype=jnp.int32)
    return jnp.where(jnp.arange(bands, dtype=jnp.int32) == fullest, E_DEV, counts)


def steps_of(key, extent, cuts, smallest, top_value):
    factor_of = 1.0
    for position, parts in cuts:
        steps = jax.random.uniform(jax.random.fold_in(jax.random.fold_in(key, 6), position), (parts,), jnp.float32, smallest / len(cuts), top_value / len(cuts))
        factor_of = factor_of * jnp.repeat(jnp.exp(steps), extent[position] // parts).reshape((-1,) + (1,) * (len(extent) - 1 - position))
    return factor_of


def normal_values(stream_key, shape, scale, reach, cuts=(), kind=jnp.bfloat16):
    drawn = jax.random.normal(stream_key, shape, jnp.float32) * scale
    if len(cuts) > 0:
        drawn = steps_of(stream_key, shape, cuts, -0.22, 0.18) * drawn
    return jnp.clip(drawn, min=-reach, max=reach).astype(kind)


def setup_inputs(seed: int = 0) -> dict:
    arg_keys = jax.random.split(jax.random.key(seed), 13)
    return {
        "grid_latent": normal_values(arg_keys[0], (GRID, D), 1.0, 6.0, ((0, 256),)),
        "edge_latent": normal_values(arg_keys[1], (EDGES, D), 1.0, 6.0, ((0, 256),)),
        "mesh_latent": normal_values(arg_keys[2], (MESH, D), 1.0, 6.0, ((0, 256),)),
        "mesh_cotangent": normal_values(arg_keys[3], (MESH, D), 1.0, 6.0, ((0, 256),)),
        "w_grid": normal_values(arg_keys[4], (D, H), (3 * D) ** -0.5, 0.15625, ((1, 2),)),
        "w_mesh": normal_values(arg_keys[5], (D, H), (3 * D) ** -0.5, 0.15625, ((1, 2),)),
        "w_edge": normal_values(arg_keys[6], (D, H), (3 * D) ** -0.5, 0.15625, ((1, 2),)),
        "bias": normal_values(arg_keys[7], (H,), 0.7, 3.0, ((0, 2),), jnp.float32),
        "w_out": normal_values(arg_keys[8], (H, D), H ** -0.5, 0.25, ((0, 2),)),
        "senders": draw_senders(jax.random.fold_in(arg_keys[12], 71), 0),
        "receivers": draw_receivers(jax.random.fold_in(arg_keys[12], 71), 0),
        "edge_count": draw_edge_count(jax.random.fold_in(arg_keys[12], 71), 0),
    }


def reference(grid_latent, edge_latent, mesh_latent, mesh_cotangent, w_grid, w_mesh, w_edge, bias, w_out, senders, receivers, edge_count):
    rows = jnp.arange(EDGES, dtype=jnp.int32)
    live = (rows % E_DEV) < edge_count[rows // E_DEV]
    gsend = grid_latent[senders]
    mrecv = mesh_latent[receivers]
    pre = (jnp.dot(gsend, w_grid, preferred_element_type=jnp.float32)
           + jnp.dot(mrecv, w_mesh, preferred_element_type=jnp.float32)
           + jnp.dot(edge_latent, w_edge, preferred_element_type=jnp.float32) + bias)
    sig = jax.nn.sigmoid(pre)
    act = (pre * sig).astype(jnp.bfloat16)
    message_cot = jnp.where(live[:, None], mesh_cotangent[receivers], jnp.zeros((), jnp.bfloat16))
    hidden_cot = jnp.dot(message_cot, w_out.T, preferred_element_type=jnp.float32)
    pre_cot = (hidden_cot * sig * (1.0 + pre * (1.0 - sig))).astype(jnp.bfloat16)
    grad_w_grid = jnp.dot(gsend.T, pre_cot, preferred_element_type=jnp.float32)
    grad_w_mesh = jnp.dot(mrecv.T, pre_cot, preferred_element_type=jnp.float32)
    grad_w_edge = jnp.dot(edge_latent.T, pre_cot, preferred_element_type=jnp.float32)
    grad_w_out = jnp.dot(act.T, message_cot, preferred_element_type=jnp.float32)
    grad_bias = jnp.sum(pre_cot.astype(jnp.float32), axis=0)
    group = H // N_CHAN
    edge_total = jnp.zeros((EDGES, D), jnp.float32)
    grid_total = jnp.zeros((GRID, D), jnp.float32)
    for index in range(N_CHAN):
        part_cot = pre_cot[:, index * group:(index + 1) * group]
        edge_part = jnp.dot(part_cot, w_edge[:, index * group:(index + 1) * group].T, preferred_element_type=jnp.float32)
        edge_part = lax.optimization_barrier(edge_part.astype(jnp.bfloat16))
        edge_total = edge_total + edge_part.astype(jnp.float32)
        grid_part = jnp.dot(part_cot, w_grid[:, index * group:(index + 1) * group].T, preferred_element_type=jnp.float32)
        grid_part = jax.ops.segment_sum(grid_part, senders, num_segments=GRID)
        grid_part = lax.optimization_barrier(grid_part.astype(jnp.bfloat16))
        grid_total = grid_total + grid_part.astype(jnp.float32)
    mesh_terms = jnp.dot(pre_cot, w_mesh.T, preferred_element_type=jnp.float32)
    grad_mesh = jax.ops.segment_sum(mesh_terms, receivers, num_segments=MESH).astype(jnp.bfloat16)
    return (grid_total.astype(jnp.bfloat16), edge_total.astype(jnp.bfloat16), grad_mesh,
            grad_w_grid, grad_w_mesh, grad_w_edge, grad_bias, grad_w_out)
```

```python
import functools

import jax
import jax.numpy as jnp
import numpy as np
from jax import lax
from jax.experimental import pallas as pl
from jax.experimental.pallas import tpu as pltpu
from jax.sharding import Mesh, PartitionSpec as P

BF = jnp.bfloat16
F32 = jnp.float32
BAND = ("z", "y", "x")
PLANE = ("y", "x")
LANES = 128
EDGE_BLOCK = 384
TAIL = 16


def dot(a, b):
    return jnp.dot(a, b, preferred_element_type=F32)


def dot_t(a, b):
    return lax.dot_general(a, b, (((1,), (1,)), ((), ())), preferred_element_type=F32)


def dot_rows(a, b):
    return lax.dot_general(a, b, (((0,), (0,)), ((), ())), preferred_element_type=F32)


def edge_kernel(
    grid_own,
    grid_far,
    edge_own,
    edge_far,
    m0,
    m1,
    m2,
    m3,
    m4,
    m5,
    w_grid,
    w_mesh,
    w_edge,
    w_out,
    bias,
    send_col,
    recv_col,
    send_row,
    recv_row,
    wire,
    cot_own,
    cot_far,
    seg_grid,
    rim_low,
    rim_mid,
    rim_high,
    lat,
    cot,
    table,
    cot_table,
    left,
    right,
    sums,
    act_sums,
    edge_sum,
    bias_sum,
):
    half_edges = edge_own.shape[0]
    half_grid = grid_own.shape[0]
    n_grid = 2 * half_grid
    piece = m0.shape[1]
    n_mesh = 6 * piece
    pad_mesh = lat.shape[0]
    n_rows = n_grid + pad_mesh
    block = left.shape[0]
    hidden = w_grid.shape[1]
    for k, m in enumerate((m0, m1, m2, m3, m4, m5)):
        lat[k * piece : (k + 1) * piece] = m[0]
        cot[k * piece : (k + 1) * piece] = m[1]
    if pad_mesh > n_mesh:
        lat[n_mesh:] = jnp.zeros((pad_mesh - n_mesh, lat.shape[1]), BF)
        cot[n_mesh:] = jnp.zeros((pad_mesh - n_mesh, cot.shape[1]), BF)
    table[0:half_grid] = dot(grid_own[...], w_grid[...]).astype(BF)
    table[half_grid:n_grid] = dot(grid_far[...], w_grid[...]).astype(BF)
    table[n_grid:n_rows] = dot(lat[...], w_mesh[...]).astype(BF)
    table[n_rows:] = w_edge[...]
    cot_table[...] = dot_t(cot[...], w_out[...]).astype(BF)
    sums[...] = jnp.zeros_like(sums)
    act_sums[...] = jnp.zeros_like(act_sums)
    edge_sum[...] = jnp.zeros_like(edge_sum)
    bias_sum[...] = jnp.zeros_like(bias_sum)

    def run(edges, cot_out, base):
        def step(i, carry):
            at = pl.multiple_of(i * block, block)
            rows = pl.ds(at, block)
            wide = pl.ds(pl.multiple_of(base + at, block), block)
            lane = lax.broadcasted_iota(jnp.int32, (block, LANES), 1)
            sender = send_col[wide, :]
            receiver = recv_col[wide, :]
            for k in range(n_grid // LANES):
                left[:, k * LANES : (k + 1) * LANES] = jnp.where(sender == lane + k * LANES, 1.0, 0.0).astype(BF)
            for k in range(pad_mesh // LANES):
                at_lane = n_grid + k * LANES
                left[:, at_lane : at_lane + LANES] = jnp.where(receiver == lane + k * LANES, 1.0, 0.0).astype(BF)
            left[:, n_rows:] = edges[rows, :]
            pre = dot(left[...], table[...]) + bias[...]
            hidden_cot = dot(left[:, n_grid:n_rows], cot_table[...])
            sig = jax.nn.sigmoid(pre)
            act = (pre * sig).astype(BF)
            pre_cot = (hidden_cot * sig * (1.0 + pre * (1.0 - sig))).astype(BF)
            cot_out[rows, :] = pre_cot
            sub = lax.broadcasted_iota(jnp.int32, (LANES, block), 0)
            sender_row = jnp.broadcast_to(send_row[:, wide], (LANES, block))
            receiver_row = jnp.broadcast_to(recv_row[:, wide], (LANES, block))
            for k in range(n_grid // LANES):
                right[k * LANES : (k + 1) * LANES, :] = jnp.where(sender_row == sub + k * LANES, 1.0, 0.0).astype(BF)
            for k in range(pad_mesh // LANES):
                at_row = n_grid + k * LANES
                right[at_row : at_row + LANES, :] = jnp.where(receiver_row == sub + k * LANES, 1.0, 0.0).astype(BF)
            sums[...] += dot(right[...], pre_cot)
            act_sums[...] += dot(right[n_grid:, :], act)
            edge_sum[...] += dot_rows(edges[rows, :], pre_cot)
            bias_sum[...] += jnp.sum(pre_cot.astype(F32), axis=0, keepdims=True)
            return carry

        lax.fori_loop(0, half_edges // block, step, 0)

    run(edge_own, cot_own, 0)
    run(edge_far, cot_far, half_edges)

    seg_grid[...] = sums[:n_grid].astype(BF)
    seg_mesh = sums[n_grid:].astype(BF)
    grads = (
        dot_rows(grid_own[...], seg_grid[:half_grid]) + dot_rows(grid_far[...], seg_grid[half_grid:]),
        dot_rows(lat[...], seg_mesh),
        edge_sum[...],
    )
    rows = 128
    at = 0

    def put(at, value):
        wire[at, 0:rows, :] = value[:, :LANES].astype(BF)
        wire[at, rows : 2 * rows, :] = value[:, LANES:].astype(BF)

    for g in grads:
        for k in range(g.shape[0] // rows):
            put(at, g[k * rows : (k + 1) * rows])
            at += 1
    g = dot_rows(act_sums[...].astype(BF), cot[...])
    for c in range(2):
        for k in range(g.shape[0] // rows):
            put(at, g[k * rows : (k + 1) * rows, c * hidden : (c + 1) * hidden])
            at += 1
    sub = lax.broadcasted_iota(jnp.int32, (TAIL, LANES), 0)
    low = jnp.broadcast_to(bias_sum[:, :LANES], (TAIL, LANES))
    high = jnp.broadcast_to(bias_sum[:, LANES:], (TAIL, LANES))
    tail = jnp.where(sub == 0, low, jnp.where(sub == 1, high, 0.0)).astype(BF)
    for k in range(wire.shape[0]):
        wire[k, 2 * rows :, :] = tail
    for ref, o, kind in ((rim_low, 0, BF), (rim_mid, 1, F32), (rim_high, 2, BF)):
        for h in range(2):
            start = n_grid + (3 * h + o) * piece
            ref[h * piece : (h + 1) * piece] = sums[start : start + piece].astype(kind)


def swap(x):
    return lax.ppermute(x, "chan", [(0, 1), (1, 0)])


def shifted(x, by):
    n = lax.axis_size(BAND)
    return lax.ppermute(x, BAND, [(i, i + by) for i in range(n) if 0 <= i + by < n])


def plane_total(wire):
    arrived = lax.all_to_all(wire, PLANE, 0, 0, tiled=True)
    total = arrived.astype(F32).sum(axis=0)
    depth = lax.axis_size("z")
    step = 1
    while step < depth:
        mine = total.astype(BF)
        other = lax.ppermute(mine, "z", [(i, i ^ step) for i in range(depth)])
        total = mine.astype(F32) + other.astype(F32)
        step *= 2
    chunk = total[:-TAIL].astype(BF)
    bias_total = total[-TAIL:]
    members = wire.shape[0]
    everyone = lax.all_to_all(jnp.broadcast_to(chunk[None], (members, *chunk.shape)), PLANE, 0, 0, tiled=True)
    return everyone, bias_total


def body(
    grid_latent,
    edge_latent,
    mesh_latent,
    mesh_cotangent,
    w_grid,
    w_mesh,
    w_edge,
    bias,
    w_out,
    senders,
    receivers,
    edge_count,
):
    band = lax.axis_index(BAND)
    chan = lax.axis_index("chan")
    half_grid = grid_latent.shape[0]
    half_edges = edge_latent.shape[0]
    piece, width = mesh_latent.shape
    hidden = w_grid.shape[1]
    n_grid = 2 * half_grid
    n_edges = 2 * half_edges
    pad_mesh = -(-6 * piece // LANES) * LANES

    mesh_own = jnp.stack([mesh_latent, mesh_cotangent])
    mesh_below = shifted(mesh_own, 1)
    mesh_above = shifted(mesh_own, -1)
    edge_far = swap(edge_latent)
    grid_far = swap(grid_latent)
    mesh_near = (mesh_below, mesh_own, mesh_above)
    mesh_far = tuple(swap(m) for m in mesh_near)

    at = senders - band * n_grid - chan * half_grid
    local_send = jnp.where(at < 0, at + n_grid, at)
    at = receivers - (band - 1) * (2 * piece)
    owner = at // (2 * piece)
    within = at - owner * (2 * piece)
    half = within // piece
    local_recv = ((half ^ chan) * 3 + owner) * piece + within - half * piece
    live = jnp.arange(n_edges, dtype=jnp.int32) < edge_count[0]
    local_recv = jnp.where(live, local_recv, -1)

    def own_first(v):
        return jnp.where(chan == 0, v, jnp.concatenate([v[half_edges:], v[:half_edges]]))

    local_send = own_first(local_send)
    local_recv = own_first(local_recv)
    columns = [jnp.broadcast_to(v[:, None], (n_edges, LANES)) for v in (local_send, local_recv)]
    rows = [v.reshape(1, n_edges) for v in (local_send, local_recv)]

    members = lax.axis_size(PLANE)
    shape = jax.ShapeDtypeStruct
    vmem = pl.BlockSpec(memory_space=pltpu.VMEM)
    wire, cot_own, cot_far, seg_grid, rim_low, rim_mid, rim_high = pl.pallas_call(
        edge_kernel,
        out_shape=(
            shape((16, 256 + TAIL, LANES), BF),
            shape((half_edges, hidden), BF),
            shape((half_edges, hidden), BF),
            shape((n_grid, hidden), BF),
            shape((2 * piece, hidden), BF),
            shape((2 * piece, hidden), F32),
            shape((2 * piece, hidden), BF),
        ),
        in_specs=[vmem] * 19,
        out_specs=(vmem,) * 7,
        scratch_shapes=[
            pltpu.VMEM((pad_mesh, width), BF),
            pltpu.VMEM((pad_mesh, width), BF),
            pltpu.VMEM((n_grid + pad_mesh + width, hidden), BF),
            pltpu.VMEM((pad_mesh, hidden), BF),
            pltpu.VMEM((EDGE_BLOCK, n_grid + pad_mesh + width), BF),
            pltpu.VMEM((n_grid + pad_mesh, EDGE_BLOCK), BF),
            pltpu.VMEM((n_grid + pad_mesh, hidden), F32),
            pltpu.VMEM((pad_mesh, hidden), F32),
            pltpu.VMEM((width, hidden), F32),
            pltpu.VMEM((1, hidden), F32),
        ],
        compiler_params=pltpu.CompilerParams(vmem_limit_bytes=56 * 1024 * 1024),
        name="edge_step",
    )(
        grid_latent,
        grid_far,
        edge_latent,
        edge_far,
        *mesh_near,
        *mesh_far,
        w_grid,
        w_mesh,
        w_edge,
        w_out,
        bias.reshape(1, hidden),
        *columns,
        *rows,
    )

    from_above = shifted(rim_low, -1)
    from_below = shifted(rim_high, 1)
    edge_back = swap(dot_t(cot_far, w_edge).astype(BF))
    grid_back = swap(dot_t(seg_grid[half_grid:], w_grid).astype(BF))
    everyone, bias_total = plane_total(wire.reshape(members, -1, LANES))

    grad_edge = (dot_t(cot_own, w_edge) + edge_back.astype(F32)).astype(BF)
    grad_grid = (dot_t(seg_grid[:half_grid], w_grid) + grid_back.astype(F32)).astype(BF)
    seg_mesh = (rim_mid + from_above.astype(F32) + from_below.astype(F32)).astype(BF)
    mesh_back = swap(dot_t(seg_mesh[piece:], w_mesh).astype(BF))
    grad_mesh = (dot_t(seg_mesh[:piece], w_mesh) + mesh_back.astype(F32)).astype(BF)

    def wide(chunks):
        n = chunks.shape[0]
        pair = chunks.astype(F32).reshape(n, 2, 128, LANES)
        return jnp.concatenate([pair[:, 0], pair[:, 1]], axis=-1).reshape(n * 128, 2 * LANES)

    grad_w_grid = wide(everyone[0:4])
    grad_w_mesh = wide(everyone[4:8])
    grad_w_edge = wide(everyone[8:12])
    grad_w_out = jnp.concatenate([wide(everyone[12:14]), wide(everyone[14:16])], axis=1)
    grad_bias = jnp.concatenate([bias_total[0], bias_total[1]])
    return (
        grad_grid,
        grad_edge,
        grad_mesh,
        grad_w_grid,
        grad_w_mesh,
        grad_w_edge,
        grad_bias,
        grad_w_out,
    )


def solution(mesh):
    bands, chans = (mesh.shape["band"], mesh.shape["chan"])
    side = 4
    inner = Mesh(np.asarray(mesh.devices).reshape(bands // side**2, side, side, chans), (*BAND, "chan"))
    every = P((*BAND, "chan"), None)
    return jax.shard_map(
        body,
        mesh=inner,
        in_specs=(
            every,
            every,
            every,
            every,
            P(None, "chan"),
            P(None, "chan"),
            P(None, "chan"),
            P("chan"),
            P("chan", None),
            P(BAND),
            P(BAND),
            P(BAND),
        ),
        out_specs=(
            every,
            every,
            every,
            P(None, "chan"),
            P(None, "chan"),
            P(None, "chan"),
            P("chan"),
            P("chan", None),
        ),
        check_vma=False,
    )
```

```python
import functools

import jax
import jax.numpy as jnp
import numpy as np
from jax import lax
from jax.experimental import pallas as pl
from jax.experimental.pallas import tpu as pltpu
from jax.sharding import Mesh, PartitionSpec as P

BF = jnp.bfloat16
F32 = jnp.float32
BAND = ("z", "y", "x")
PLANE = ("y", "x")
LANES = 128
EDGE_BLOCK = 384
TAIL = 16
SENDER_FLOPS = 4 * 10**9
EDGE_FLOPS = 9 * 10**9


def dot(a, b):
    return jnp.dot(a, b, preferred_element_type=F32)


def dot_t(a, b):
    return lax.dot_general(a, b, (((1,), (1,)), ((), ())), preferred_element_type=F32)


def dot_rows(a, b):
    return lax.dot_general(a, b, (((0,), (0,)), ((), ())), preferred_element_type=F32)


def one_hot(column, offset):
    place = lax.broadcasted_iota(jnp.int32, column.shape, column.ndim - 1)
    return jnp.where(column == place + offset, 1.0, 0.0).astype(BF)


def one_hot_rows(row, offset):
    place = lax.broadcasted_iota(jnp.int32, row.shape, 0)
    return jnp.where(row == place + offset, 1.0, 0.0).astype(BF)


def local_senders(row, where, half_grid):
    at = row - where[0] * (2 * half_grid) - where[1] * half_grid
    return jnp.where(at < 0, at + 2 * half_grid, at)


def local_receivers(row, slot, where, piece):
    at = row - (where[0] - 1) * (2 * piece)
    owner = jnp.where(at >= 2 * piece, 1, 0) + jnp.where(at >= 4 * piece, 1, 0)
    within = at - owner * (2 * piece)
    half = jnp.where(within >= piece, 1, 0)
    flip = jnp.where(half == where[1], 0, 1)
    near = (flip * 3 + owner) * piece + within - half * piece
    return jnp.where(slot < where[2], near, -1)


def sender_kernel(
    where, grid_own, grid_far, edge_own, edge_far, w_grid, w_edge, bias, senders, pre_own, pre_far, table, left
):
    half_edges = edge_own.shape[0]
    half_grid = grid_own.shape[0]
    n_grid = 2 * half_grid
    block = left.shape[0]
    table[0:half_grid] = dot(grid_own[...], w_grid[...]).astype(BF)
    table[half_grid:n_grid] = dot(grid_far[...], w_grid[...]).astype(BF)
    table[n_grid:] = w_edge[...]
    parts = half_edges // LANES

    def run(edges, pre, base):
        def step(i, carry):
            rows = pl.ds(pl.multiple_of(i * block, block), block)
            for c in range(block // LANES):
                at = base + i * (block // LANES) + c
                row = local_senders(senders[pl.ds(at, 1), :], where, half_grid)
                column = jnp.broadcast_to(row, (LANES, LANES)).T
                for k in range(n_grid // LANES):
                    left[c * LANES : (c + 1) * LANES, k * LANES : (k + 1) * LANES] = one_hot(column, k * LANES)
            left[:, n_grid:] = edges[rows, :]
            pre[rows, :] = dot(left[...], table[...]) + bias[...]
            return carry

        lax.fori_loop(0, half_edges // block, step, 0)

    run(edge_own, pre_own, where[1] * parts)
    run(edge_far, pre_far, (1 - where[1]) * parts)


def edge_kernel(
    where,
    grid_own,
    grid_far,
    edge_own,
    edge_far,
    m0,
    m1,
    m2,
    m3,
    m4,
    m5,
    w_mesh,
    w_out,
    pre_own,
    pre_far,
    senders,
    receivers,
    wire,
    cot_own,
    cot_far,
    seg_grid,
    rim_low,
    rim_mid,
    rim_high,
    lat,
    cot,
    table,
    left,
    right,
    sums,
    act_sums,
    edge_sum,
    bias_sum,
):
    half_edges = edge_own.shape[0]
    half_grid = grid_own.shape[0]
    n_grid = 2 * half_grid
    piece = m0.shape[1]
    n_mesh = 6 * piece
    pad_mesh = lat.shape[0]
    n_rows = n_grid + pad_mesh
    block = left.shape[0]
    hidden = w_mesh.shape[1]
    for k, m in enumerate((m0, m1, m2, m3, m4, m5)):
        lat[k * piece : (k + 1) * piece] = m[0]
        cot[k * piece : (k + 1) * piece] = m[1]
    if pad_mesh > n_mesh:
        lat[n_mesh:] = jnp.zeros((pad_mesh - n_mesh, lat.shape[1]), BF)
        cot[n_mesh:] = jnp.zeros((pad_mesh - n_mesh, cot.shape[1]), BF)
    table[:, 0:hidden] = dot(lat[...], w_mesh[...]).astype(BF)
    cots = dot_t(cot[...], w_out[...])
    high = cots.astype(BF)
    table[:, hidden : 2 * hidden] = high
    table[:, 2 * hidden :] = (cots - high.astype(F32)).astype(BF)
    sums[...] = jnp.zeros_like(sums)
    act_sums[...] = jnp.zeros_like(act_sums)
    edge_sum[...] = jnp.zeros_like(edge_sum)
    bias_sum[...] = jnp.zeros_like(bias_sum)
    parts = half_edges // LANES

    def run(edges, pre_part, cot_out, base):
        def step(i, carry):
            rows = pl.ds(pl.multiple_of(i * block, block), block)
            for c in range(block // LANES):
                at = base + i * (block // LANES) + c
                mine = slice(c * LANES, (c + 1) * LANES)
                slot = at * LANES + lax.broadcasted_iota(jnp.int32, (1, LANES), 1)
                row = local_receivers(receivers[pl.ds(at, 1), :], slot, where, piece)
                row = jnp.broadcast_to(row, (LANES, LANES))
                column = row.T
                for k in range(pad_mesh // LANES):
                    left[mine, k * LANES : (k + 1) * LANES] = one_hot(column, k * LANES)
                    at_row = n_grid + k * LANES
                    right[at_row : at_row + LANES, mine] = one_hot_rows(row, k * LANES)
                row = local_senders(senders[pl.ds(at, 1), :], where, half_grid)
                row = jnp.broadcast_to(row, (LANES, LANES))
                for k in range(n_grid // LANES):
                    right[k * LANES : (k + 1) * LANES, mine] = one_hot_rows(row, k * LANES)
            got = dot(left[...], table[...])
            pre = pre_part[rows, :] + got[:, 0:hidden]
            hidden_cot = got[:, hidden : 2 * hidden] + got[:, 2 * hidden :]
            sig = jax.nn.sigmoid(pre)
            act = (pre * sig).astype(BF)
            pre_cot = (hidden_cot * sig * (1.0 + pre * (1.0 - sig))).astype(BF)
            cot_out[rows, :] = pre_cot
            sums[...] += dot(right[...], pre_cot)
            act_sums[...] += dot(right[n_grid:, :], act)
            edge_sum[...] += dot_rows(edges[rows, :], pre_cot)
            bias_sum[...] += jnp.sum(pre_cot.astype(F32), axis=0, keepdims=True)
            return carry

        lax.fori_loop(0, half_edges // block, step, 0)

    run(edge_own, pre_own, cot_own, where[1] * parts)
    run(edge_far, pre_far, cot_far, (1 - where[1]) * parts)

    seg_grid[...] = sums[:n_grid].astype(BF)
    seg_mesh = sums[n_grid:].astype(BF)
    grads = (
        dot_rows(grid_own[...], seg_grid[:half_grid]) + dot_rows(grid_far[...], seg_grid[half_grid:]),
        dot_rows(lat[...], seg_mesh),
        edge_sum[...],
    )
    rows = 128
    at = 0

    def put(at, value):
        wire[at, 0:rows, :] = value[:, :LANES].astype(BF)
        wire[at, rows : 2 * rows, :] = value[:, LANES:].astype(BF)

    for g in grads:
        for k in range(g.shape[0] // rows):
            put(at, g[k * rows : (k + 1) * rows])
            at += 1
    g = dot_rows(act_sums[...].astype(BF), cot[...])
    for c in range(2):
        for k in range(g.shape[0] // rows):
            put(at, g[k * rows : (k + 1) * rows, c * hidden : (c + 1) * hidden])
            at += 1
    sub = lax.broadcasted_iota(jnp.int32, (TAIL, LANES), 0)
    low = jnp.broadcast_to(bias_sum[:, :LANES], (TAIL, LANES))
    high = jnp.broadcast_to(bias_sum[:, LANES:], (TAIL, LANES))
    tail = jnp.where(sub == 0, low, jnp.where(sub == 1, high, 0.0)).astype(BF)
    for k in range(wire.shape[0]):
        wire[k, 2 * rows :, :] = tail
    for ref, o, kind in ((rim_low, 0, BF), (rim_mid, 1, F32), (rim_high, 2, BF)):
        for h in range(2):
            start = n_grid + (3 * h + o) * piece
            ref[h * piece : (h + 1) * piece] = sums[start : start + piece].astype(kind)


def last_sum_kernel(mine, other, spread, bias):
    total = mine[...].astype(F32) + other[...].astype(F32)
    rows = spread.shape[1]
    low, high = (total[:rows].astype(BF), total[rows : 2 * rows].astype(BF))
    for k in range(spread.shape[0]):
        spread[k, :, :LANES] = low
        spread[k, :, LANES:] = high
    bias[:, :LANES] = total[2 * rows : 2 * rows + 1]
    bias[:, LANES:] = total[2 * rows + 1 : 2 * rows + 2]


def swap(x):
    return lax.ppermute(x, "chan", [(0, 1), (1, 0)])


def shifted(x, by):
    n = lax.axis_size(BAND)
    return lax.ppermute(x, BAND, [(i, i + by) for i in range(n) if 0 <= i + by < n])


def depth_total(mine):
    depth = lax.axis_size("z")
    step = 1
    while True:
        other = lax.ppermute(mine, "z", [(i, i ^ step) for i in range(depth)])
        step *= 2
        if step == depth:
            return mine, other
        mine = (mine.astype(F32) + other.astype(F32)).astype(BF)


def body(
    grid_latent,
    edge_latent,
    mesh_latent,
    mesh_cotangent,
    w_grid,
    w_mesh,
    w_edge,
    bias,
    w_out,
    senders,
    receivers,
    edge_count,
):
    band = lax.axis_index(BAND)
    chan = lax.axis_index("chan")
    half_grid = grid_latent.shape[0]
    half_edges = edge_latent.shape[0]
    piece, width = mesh_latent.shape
    hidden = w_grid.shape[1]
    n_grid = 2 * half_grid
    pad_mesh = -(-6 * piece // LANES) * LANES

    mesh_own = jnp.stack([mesh_latent, mesh_cotangent])
    mesh_below = shifted(mesh_own, 1)
    mesh_above = shifted(mesh_own, -1)
    edge_far = swap(edge_latent)
    grid_far = swap(grid_latent)
    mesh_own_far = swap(mesh_own)

    where = jnp.stack([band, chan, edge_count[0]])
    senders = senders.reshape(-1, LANES)
    receivers = receivers.reshape(-1, LANES)
    shape = jax.ShapeDtypeStruct
    vmem = pl.BlockSpec(memory_space=pltpu.VMEM)
    smem = pl.BlockSpec(memory_space=pltpu.SMEM)
    params = pltpu.CompilerParams(vmem_limit_bytes=56 * 1024 * 1024)
    pre_own, pre_far = pl.pallas_call(
        sender_kernel,
        out_shape=(shape((half_edges, hidden), F32),) * 2,
        in_specs=[smem] + [vmem] * 8,
        out_specs=(vmem,) * 2,
        scratch_shapes=[
            pltpu.VMEM((n_grid + width, hidden), BF),
            pltpu.VMEM((EDGE_BLOCK, n_grid + width), BF),
        ],
        compiler_params=params,
        cost_estimate=pl.CostEstimate(flops=SENDER_FLOPS, transcendentals=0, bytes_accessed=1 << 22),
        name="sender_step",
    )(where, grid_latent, grid_far, edge_latent, edge_far, w_grid, w_edge, bias.reshape(1, hidden), senders)

    mesh_below, mesh_above, pre_own, pre_far = lax.optimization_barrier((mesh_below, mesh_above, pre_own, pre_far))
    mesh_near = (mesh_below, mesh_own, mesh_above)
    mesh_far = (swap(mesh_below), mesh_own_far, swap(mesh_above))
    wire, cot_own, cot_far, seg_grid, rim_low, rim_mid, rim_high = pl.pallas_call(
        edge_kernel,
        out_shape=(
            shape((16, 256 + TAIL, LANES), BF),
            shape((half_edges, hidden), BF),
            shape((half_edges, hidden), BF),
            shape((n_grid, hidden), BF),
            shape((2 * piece, hidden), BF),
            shape((2 * piece, hidden), F32),
            shape((2 * piece, hidden), BF),
        ),
        in_specs=[smem] + [vmem] * 16,
        out_specs=(vmem,) * 7,
        scratch_shapes=[
            pltpu.VMEM((pad_mesh, width), BF),
            pltpu.VMEM((pad_mesh, width), BF),
            pltpu.VMEM((pad_mesh, 3 * hidden), BF),
            pltpu.VMEM((EDGE_BLOCK, pad_mesh), BF),
            pltpu.VMEM((n_grid + pad_mesh, EDGE_BLOCK), BF),
            pltpu.VMEM((n_grid + pad_mesh, hidden), F32),
            pltpu.VMEM((pad_mesh, hidden), F32),
            pltpu.VMEM((width, hidden), F32),
            pltpu.VMEM((1, hidden), F32),
        ],
        compiler_params=params,
        cost_estimate=pl.CostEstimate(flops=EDGE_FLOPS, transcendentals=1 << 20, bytes_accessed=1 << 23),
        name="edge_step",
    )(
        where,
        grid_latent,
        grid_far,
        edge_latent,
        edge_far,
        *mesh_near,
        *mesh_far,
        w_mesh,
        w_out,
        pre_own,
        pre_far,
        senders,
        receivers,
    )

    arrived = lax.all_to_all(wire, PLANE, 0, 0, tiled=True)
    edge_term = dot_t(cot_far, w_edge).astype(BF)
    grid_term = dot_t(seg_grid[half_grid:], w_grid).astype(BF)
    edge_back = swap(edge_term)
    grid_back = swap(grid_term)
    total = arrived.astype(F32).sum(axis=0).astype(BF)
    total, rim_low, rim_high, _, _ = lax.optimization_barrier((total, rim_low, rim_high, edge_term, grid_term))
    from_above = shifted(rim_low, -1)
    from_below = shifted(rim_high, 1)
    mine, other = depth_total(total)
    spread, grad_bias = pl.pallas_call(
        last_sum_kernel,
        out_shape=(shape((16, 128, hidden), BF), shape((1, hidden), F32)),
        in_specs=[vmem] * 2,
        out_specs=(vmem,) * 2,
        name="last_sum",
    )(mine, other)
    everyone = lax.all_to_all(spread, PLANE, 0, 0, tiled=True)

    rim_mid, from_above, from_below, _ = lax.optimization_barrier((rim_mid, from_above, from_below, grad_bias))
    grad_edge = (dot_t(cot_own, w_edge) + edge_back.astype(F32)).astype(BF)
    grad_grid = (dot_t(seg_grid[:half_grid], w_grid) + grid_back.astype(F32)).astype(BF)
    seg_mesh = (rim_mid + from_above.astype(F32) + from_below.astype(F32)).astype(BF)
    mesh_back = swap(dot_t(seg_mesh[piece:], w_mesh).astype(BF))
    grad_mesh = (dot_t(seg_mesh[:piece], w_mesh) + mesh_back.astype(F32)).astype(BF)

    def rows_of(start, stop):
        return everyone[start:stop].astype(F32).reshape(-1, hidden)

    return (
        grad_grid,
        grad_edge,
        grad_mesh,
        rows_of(0, 4),
        rows_of(4, 8),
        rows_of(8, 12),
        grad_bias.reshape(hidden),
        jnp.concatenate([rows_of(12, 14), rows_of(14, 16)], axis=1),
    )


def solution(mesh):
    bands, chans = (mesh.shape["band"], mesh.shape["chan"])
    side = 4
    inner = Mesh(np.asarray(mesh.devices).reshape(bands // side**2, side, side, chans), (*BAND, "chan"))
    every = P((*BAND, "chan"), None)
    return jax.shard_map(
        body,
        mesh=inner,
        in_specs=(
            every,
            every,
            every,
            every,
            P(None, "chan"),
            P(None, "chan"),
            P(None, "chan"),
            P("chan"),
            P("chan", None),
            P(BAND),
            P(BAND),
            P(BAND),
        ),
        out_specs=(
            every,
            every,
            every,
            P(None, "chan"),
            P(None, "chan"),
            P(None, "chan"),
            P("chan"),
            P("chan", None),
        ),
        check_vma=False,
    )
```

```python
import functools

import jax
import jax.numpy as jnp
import numpy as np
from jax import lax
from jax.experimental import pallas as pl
from jax.experimental.pallas import tpu as pltpu
from jax.sharding import Mesh, PartitionSpec as P

BF = jnp.bfloat16
F32 = jnp.float32
BAND = ("z", "y", "x")
PLANE = ("y", "x")
LANES = 128
EDGE_BLOCK = 768
TAIL = 16
SENDER_FLOPS = 4 * 10**9
EDGE_FLOPS = 9 * 10**9


def dot(a, b):
    return jnp.dot(a, b, preferred_element_type=F32)


def dot_t(a, b):
    return lax.dot_general(a, b, (((1,), (1,)), ((), ())), preferred_element_type=F32)


def dot_rows(a, b):
    return lax.dot_general(a, b, (((0,), (0,)), ((), ())), preferred_element_type=F32)


def one_hot(column, offset):
    place = lax.broadcasted_iota(jnp.int32, column.shape, column.ndim - 1)
    return jnp.where(column == place + offset, 1.0, 0.0).astype(BF)


def one_hot_rows(row, offset):
    place = lax.broadcasted_iota(jnp.int32, row.shape, 0)
    return jnp.where(row == place + offset, 1.0, 0.0).astype(BF)


def local_senders(row, where, half_grid):
    at = row - where[0] * (2 * half_grid) - where[1] * half_grid
    return jnp.where(at < 0, at + 2 * half_grid, at)


def local_receivers(row, slot, where, piece):
    at = row - (where[0] - 1) * (2 * piece)
    owner = jnp.where(at >= 2 * piece, 1, 0) + jnp.where(at >= 4 * piece, 1, 0)
    within = at - owner * (2 * piece)
    half = jnp.where(within >= piece, 1, 0)
    flip = jnp.where(half == where[1], 0, 1)
    place = jnp.where(where[0] % 2 == 0, 2 - owner, owner)
    near = (flip * 3 + place) * piece + within - half * piece
    return jnp.where(slot < where[2], near, -1)


def index_row(group, groups, where):
    at = group + where[1] * (groups // 2)
    return jnp.where(at >= groups, at - groups, at)


def copies(pairs, sems):
    return [pltpu.make_async_copy(src, dst, sems.at[k]) for k, (src, dst) in enumerate(pairs)]


def sender_kernel(
    where,
    grid_own,
    grid_far,
    edge_own,
    edge_far,
    w_grid,
    w_edge,
    bias,
    senders,
    pre_out,
    grid,
    edge,
    pre,
    table,
    left,
    in_sems,
    out_sems,
):
    half_edges = edge_own.shape[0]
    half_grid = grid_own.shape[0]
    n_grid = 2 * half_grid
    block = left.shape[0]
    fetches = copies(
        (
            (grid_own, grid.at[0:half_grid]),
            (grid_far, grid.at[half_grid:]),
            (edge_own, edge.at[0:half_edges]),
            (edge_far, edge.at[half_edges:]),
        ),
        in_sems,
    )
    for f in fetches:
        f.start()
    table[n_grid:] = w_edge[...]
    fetches[0].wait()
    fetches[1].wait()
    table[0:n_grid] = dot(grid[...], w_grid[...]).astype(BF)
    fetches[2].wait()
    fetches[3].wait()
    groups = 2 * half_edges // LANES
    per = block // LANES
    steps = 2 * half_edges // block

    def step(i, carry):
        rows = pl.ds(pl.multiple_of(i * block, block), block)
        for c in range(per):
            at = index_row(i * per + c, groups, where)
            row = local_senders(senders[pl.ds(at, 1), :], where, half_grid)
            column = jnp.broadcast_to(row, (LANES, LANES)).T
            for k in range(n_grid // LANES):
                left[c * LANES : (c + 1) * LANES, k * LANES : (k + 1) * LANES] = one_hot(column, k * LANES)
        left[:, n_grid:] = edge[rows, :]
        pre[rows, :] = dot(left[...], table[...]) + bias[...]
        pltpu.make_async_copy(pre.at[rows], pre_out.at[rows], out_sems.at[i]).start()
        return carry

    lax.fori_loop(0, steps, step, 0)
    for k in range(steps):
        rows = pl.ds(k * block, block)
        pltpu.make_async_copy(pre.at[rows], pre_out.at[rows], out_sems.at[k]).wait()


def edge_kernel(
    where,
    grid_own,
    grid_far,
    edge_own,
    edge_far,
    m0,
    m1,
    m2,
    m3,
    m4,
    m5,
    w_mesh,
    w_out,
    pre_in,
    senders,
    receivers,
    wire_out,
    cot_own,
    cot_far,
    seg_out,
    rim_low,
    rim_mid,
    rim_high,
    grid,
    edge,
    pre_part,
    lat,
    cot,
    table,
    left,
    right,
    sums,
    act_sums,
    edge_sum,
    bias_sum,
    cots,
    seg_grid,
    wire,
    low_v,
    mid_v,
    high_v,
    in_sems,
    out_sems,
):
    half_edges = edge_own.shape[0]
    half_grid = grid_own.shape[0]
    n_grid = 2 * half_grid
    piece = m0.shape[1]
    n_mesh = 6 * piece
    pad_mesh = lat.shape[0]
    n_rows = n_grid + pad_mesh
    block = left.shape[0]
    hidden = w_mesh.shape[1]
    pieces = (m0, m1, m2, m3, m4, m5)
    lats = [(m.at[0], lat.at[k * piece : (k + 1) * piece]) for k, m in enumerate(pieces)]
    cot_pairs = [(m.at[1], cot.at[k * piece : (k + 1) * piece]) for k, m in enumerate(pieces)]
    rest = [
        (pre_in, pre_part),
        (edge_own, edge.at[0:half_edges]),
        (edge_far, edge.at[half_edges:]),
        (grid_own, grid.at[0:half_grid]),
        (grid_far, grid.at[half_grid:]),
    ]
    fetches = copies(lats + cot_pairs + rest, in_sems)
    for f in fetches:
        f.start()
    if pad_mesh > n_mesh:
        lat[n_mesh:] = jnp.zeros((pad_mesh - n_mesh, lat.shape[1]), BF)
        cot[n_mesh:] = jnp.zeros((pad_mesh - n_mesh, cot.shape[1]), BF)
    sums[...] = jnp.zeros_like(sums)
    act_sums[...] = jnp.zeros_like(act_sums)
    edge_sum[...] = jnp.zeros_like(edge_sum)
    bias_sum[...] = jnp.zeros_like(bias_sum)
    for f in fetches[0:12]:
        f.wait()
    table[:, 0:hidden] = dot(lat[...], w_mesh[...]).astype(BF)
    cot_terms = dot_t(cot[...], w_out[...])
    high = cot_terms.astype(BF)
    table[:, hidden : 2 * hidden] = high
    table[:, 2 * hidden :] = (cot_terms - high.astype(F32)).astype(BF)
    for f in fetches[12:]:
        f.wait()
    groups = 2 * half_edges // LANES
    per = block // LANES

    def step(i, carry):
        rows = pl.ds(pl.multiple_of(i * block, block), block)
        for c in range(per):
            at = index_row(i * per + c, groups, where)
            mine = slice(c * LANES, (c + 1) * LANES)
            slot = at * LANES + lax.broadcasted_iota(jnp.int32, (1, LANES), 1)
            row = local_receivers(receivers[pl.ds(at, 1), :], slot, where, piece)
            row = jnp.broadcast_to(row, (LANES, LANES))
            column = row.T
            for k in range(pad_mesh // LANES):
                left[mine, k * LANES : (k + 1) * LANES] = one_hot(column, k * LANES)
                at_row = n_grid + k * LANES
                right[at_row : at_row + LANES, mine] = one_hot_rows(row, k * LANES)
            row = local_senders(senders[pl.ds(at, 1), :], where, half_grid)
            row = jnp.broadcast_to(row, (LANES, LANES))
            for k in range(n_grid // LANES):
                right[k * LANES : (k + 1) * LANES, mine] = one_hot_rows(row, k * LANES)
        got = dot(left[...], table[...])
        pre = pre_part[rows, :] + got[:, 0:hidden]
        hidden_cot = got[:, hidden : 2 * hidden] + got[:, 2 * hidden :]
        sig = jax.nn.sigmoid(pre)
        act = (pre * sig).astype(BF)
        pre_cot = (hidden_cot * sig * (1.0 + pre * (1.0 - sig))).astype(BF)
        cots[rows, :] = pre_cot
        sums[...] += dot(right[...], pre_cot)
        act_sums[...] += dot(right[n_grid:, :], act)
        edge_sum[...] += dot_rows(edge[rows, :], pre_cot)
        bias_sum[...] += jnp.sum(pre_cot.astype(F32), axis=0, keepdims=True)
        return carry

    lax.fori_loop(0, 2 * half_edges // block, step, 0)

    seg_grid[...] = sums[:n_grid].astype(BF)
    for ref, o, kind in ((low_v, 0, BF), (mid_v, 1, F32), (high_v, 2, BF)):
        for h in range(2):
            start = n_grid + (3 * h + o) * piece
            ref[h * piece : (h + 1) * piece] = sums[start : start + piece].astype(kind)
    stores = copies(
        (
            (low_v, rim_low),
            (high_v, rim_high),
            (seg_grid, seg_out),
            (cots.at[0:half_edges], cot_own),
            (cots.at[half_edges:], cot_far),
            (mid_v, rim_mid),
            (wire.at[8:12], wire_out.at[8:12]),
            (wire.at[0:4], wire_out.at[0:4]),
            (wire.at[4:8], wire_out.at[4:8]),
            (wire.at[12:16], wire_out.at[12:16]),
        ),
        out_sems,
    )
    for f in stores[0:6]:
        f.start()
    rows = 128
    sub = lax.broadcasted_iota(jnp.int32, (TAIL, LANES), 0)
    low = jnp.broadcast_to(bias_sum[:, :LANES], (TAIL, LANES))
    high = jnp.broadcast_to(bias_sum[:, LANES:], (TAIL, LANES))
    tail = jnp.where(sub == 0, low, jnp.where(sub == 1, high, 0.0)).astype(BF)
    for k in range(wire.shape[0]):
        wire[k, 2 * rows :, :] = tail

    def put(at, value):
        wire[at, 0:rows, :] = value[:, :LANES].astype(BF)
        wire[at, rows : 2 * rows, :] = value[:, LANES:].astype(BF)

    def put_all(at, g):
        for k in range(g.shape[0] // rows):
            put(at + k, g[k * rows : (k + 1) * rows])

    put_all(8, edge_sum[...])
    stores[6].start()
    put_all(0, dot_rows(grid[...], seg_grid[...]))
    stores[7].start()
    put_all(4, dot_rows(lat[...], sums[n_grid:].astype(BF)))
    stores[8].start()
    g = dot_rows(act_sums[...].astype(BF), cot[...])
    put_all(12, g[:, 0:hidden])
    put_all(14, g[:, hidden:])
    stores[9].start()
    for f in stores:
        f.wait()


def last_sum_kernel(mine, other, spread, bias):
    total = mine[...].astype(F32) + other[...].astype(F32)
    rows = spread.shape[1]
    low, high = (total[:rows].astype(BF), total[rows : 2 * rows].astype(BF))
    for k in range(spread.shape[0]):
        spread[k, :, :LANES] = low
        spread[k, :, LANES:] = high
    bias[:, :LANES] = total[2 * rows : 2 * rows + 1]
    bias[:, LANES:] = total[2 * rows + 1 : 2 * rows + 2]


def swap(x):
    return lax.ppermute(x, "chan", [(0, 1), (1, 0)])


def pair_swap(x, first):
    n = lax.axis_size(BAND)
    pairs = [(i, i + 1) for i in range(first, n - 1, 2)]
    return lax.ppermute(x, BAND, pairs + [(j, i) for i, j in pairs])


def depth_total(mine):
    depth = lax.axis_size("z")
    step = 1
    while True:
        mask = depth - 1 if 2 * step == depth else step
        other = lax.ppermute(mine, "z", [(i, i ^ mask) for i in range(depth)])
        step *= 2
        if step == depth:
            return mine, other
        mine = (mine.astype(F32) + other.astype(F32)).astype(BF)


def body(
    grid_latent,
    edge_latent,
    mesh_latent,
    mesh_cotangent,
    w_grid,
    w_mesh,
    w_edge,
    bias,
    w_out,
    senders,
    receivers,
    edge_count,
):
    band = lax.axis_index(BAND)
    chan = lax.axis_index("chan")
    half_grid = grid_latent.shape[0]
    half_edges = edge_latent.shape[0]
    piece, width = mesh_latent.shape
    hidden = w_grid.shape[1]
    n_grid = 2 * half_grid
    pad_mesh = -(-6 * piece // LANES) * LANES

    mesh_own = jnp.stack([mesh_latent, mesh_cotangent])
    mesh_low = pair_swap(mesh_own, 0)
    mesh_high = pair_swap(mesh_own, 1)
    edge_far = swap(edge_latent)
    grid_far = swap(grid_latent)
    mesh_own_far = swap(mesh_own)

    where = jnp.stack([band, chan, edge_count[0]])
    senders = senders.reshape(-1, LANES)
    receivers = receivers.reshape(-1, LANES)
    shape = jax.ShapeDtypeStruct
    vmem = pl.BlockSpec(memory_space=pltpu.VMEM)
    smem = pl.BlockSpec(memory_space=pltpu.SMEM)
    params = pltpu.CompilerParams(vmem_limit_bytes=56 * 1024 * 1024)
    anywhere = pl.BlockSpec(memory_space=pl.ANY)
    dma = pltpu.SemaphoreType.DMA
    n_edges = 2 * half_edges
    pre = pl.pallas_call(
        sender_kernel,
        out_shape=shape((n_edges, hidden), F32),
        in_specs=[smem] + [anywhere] * 4 + [vmem] * 4,
        out_specs=anywhere,
        scratch_shapes=[
            pltpu.VMEM((n_grid, width), BF),
            pltpu.VMEM((n_edges, width), BF),
            pltpu.VMEM((n_edges, hidden), F32),
            pltpu.VMEM((n_grid + width, hidden), BF),
            pltpu.VMEM((EDGE_BLOCK, n_grid + width), BF),
            dma((4,)),
            dma((n_edges // EDGE_BLOCK,)),
        ],
        compiler_params=params,
        cost_estimate=pl.CostEstimate(flops=SENDER_FLOPS, transcendentals=0, bytes_accessed=1 << 22),
        name="sender_step",
    )(where, grid_latent, grid_far, edge_latent, edge_far, w_grid, w_edge, bias.reshape(1, hidden), senders)

    mesh_low, mesh_high, pre = lax.optimization_barrier((mesh_low, mesh_high, pre))
    mesh_near = (mesh_low, mesh_own, mesh_high)
    mesh_far = (swap(mesh_low), mesh_own_far, swap(mesh_high))
    wire, cot_own, cot_far, seg_grid, rim_low, rim_mid, rim_high = pl.pallas_call(
        edge_kernel,
        out_shape=(
            shape((16, 256 + TAIL, LANES), BF),
            shape((half_edges, hidden), BF),
            shape((half_edges, hidden), BF),
            shape((n_grid, hidden), BF),
            shape((2 * piece, hidden), BF),
            shape((2 * piece, hidden), F32),
            shape((2 * piece, hidden), BF),
        ),
        in_specs=[smem] + [anywhere] * 10 + [vmem] * 2 + [anywhere] + [vmem] * 2,
        out_specs=(anywhere,) * 7,
        scratch_shapes=[
            pltpu.VMEM((n_grid, width), BF),
            pltpu.VMEM((n_edges, width), BF),
            pltpu.VMEM((n_edges, hidden), F32),
            pltpu.VMEM((pad_mesh, width), BF),
            pltpu.VMEM((pad_mesh, width), BF),
            pltpu.VMEM((pad_mesh, 3 * hidden), BF),
            pltpu.VMEM((EDGE_BLOCK, pad_mesh), BF),
            pltpu.VMEM((n_grid + pad_mesh, EDGE_BLOCK), BF),
            pltpu.VMEM((n_grid + pad_mesh, hidden), F32),
            pltpu.VMEM((pad_mesh, hidden), F32),
            pltpu.VMEM((width, hidden), F32),
            pltpu.VMEM((1, hidden), F32),
            pltpu.VMEM((n_edges, hidden), BF),
            pltpu.VMEM((n_grid, hidden), BF),
            pltpu.VMEM((16, 256 + TAIL, LANES), BF),
            pltpu.VMEM((2 * piece, hidden), BF),
            pltpu.VMEM((2 * piece, hidden), F32),
            pltpu.VMEM((2 * piece, hidden), BF),
            dma((17,)),
            dma((10,)),
        ],
        compiler_params=params,
        cost_estimate=pl.CostEstimate(flops=EDGE_FLOPS, transcendentals=1 << 20, bytes_accessed=1 << 23),
        name="edge_step",
    )(
        where,
        grid_latent,
        grid_far,
        edge_latent,
        edge_far,
        *mesh_near,
        *mesh_far,
        w_mesh,
        w_out,
        pre,
        senders,
        receivers,
    )

    from_low = pair_swap(rim_low, 0)
    from_high = pair_swap(rim_high, 1)
    arrived = lax.all_to_all(wire, PLANE, 0, 0, tiled=True)
    edge_term = dot_t(cot_far, w_edge).astype(BF)
    grid_term = dot_t(seg_grid[half_grid:], w_grid).astype(BF)
    edge_back = swap(edge_term)
    grid_back = swap(grid_term)
    total = arrived.astype(F32).sum(axis=0).astype(BF)
    total, from_low, from_high, _, _ = lax.optimization_barrier((total, from_low, from_high, edge_term, grid_term))
    mine, other = depth_total(total)
    spread, grad_bias = pl.pallas_call(
        last_sum_kernel,
        out_shape=(shape((16, 128, hidden), BF), shape((1, hidden), F32)),
        in_specs=[vmem] * 2,
        out_specs=(vmem,) * 2,
        name="last_sum",
    )(mine, other)
    everyone = lax.all_to_all(spread, PLANE, 0, 0, tiled=True)

    grad_edge = (dot_t(cot_own, w_edge) + edge_back.astype(F32)).astype(BF)
    grad_grid = (dot_t(seg_grid[:half_grid], w_grid) + grid_back.astype(F32)).astype(BF)
    seg_mesh = (rim_mid + from_low.astype(F32) + from_high.astype(F32)).astype(BF)
    seg_mesh, _ = lax.optimization_barrier((seg_mesh, grad_bias))
    mesh_back = swap(dot_t(seg_mesh[piece:], w_mesh).astype(BF))
    grad_mesh = (dot_t(seg_mesh[:piece], w_mesh) + mesh_back.astype(F32)).astype(BF)

    def rows_of(start, stop):
        return everyone[start:stop].astype(F32).reshape(-1, hidden)

    return (
        grad_grid,
        grad_edge,
        grad_mesh,
        rows_of(0, 4),
        rows_of(4, 8),
        rows_of(8, 12),
        grad_bias.reshape(hidden),
        jnp.concatenate([rows_of(12, 14), rows_of(14, 16)], axis=1),
    )


def solution(mesh):
    bands, chans = (mesh.shape["band"], mesh.shape["chan"])
    side = 4
    inner = Mesh(np.asarray(mesh.devices).reshape(bands // side**2, side, side, chans), (*BAND, "chan"))
    every = P((*BAND, "chan"), None)
    return jax.shard_map(
        body,
        mesh=inner,
        in_specs=(
            every,
            every,
            every,
            every,
            P(None, "chan"),
            P(None, "chan"),
            P(None, "chan"),
            P("chan"),
            P("chan", None),
            P(BAND),
            P(BAND),
            P(BAND),
        ),
        out_specs=(
            every,
            every,
            every,
            P(None, "chan"),
            P(None, "chan"),
            P(None, "chan"),
            P("chan"),
            P("chan", None),
        ),
        check_vma=False,
    )
```

```python
import functools

import jax
import jax.numpy as jnp
import numpy as np
from jax import lax
from jax.experimental import pallas as pl
from jax.experimental.pallas import tpu as pltpu
from jax.sharding import Mesh, PartitionSpec as P

BF = jnp.bfloat16
F32 = jnp.float32
BAND = ("zh", "zl", "y", "x")
GROUP = ("zl", "y", "x")
LANES = 128
EDGE_BLOCK = 768
TAIL = 8
ROWS = 64
MEMBERS = 32
SENDER_FLOPS = 4 * 10**9
EDGE_FLOPS = 9 * 10**9


def dot(a, b):
    return jnp.dot(a, b, preferred_element_type=F32)


def dot_t(a, b):
    return lax.dot_general(a, b, (((1,), (1,)), ((), ())), preferred_element_type=F32)


def dot_rows(a, b):
    return lax.dot_general(a, b, (((0,), (0,)), ((), ())), preferred_element_type=F32)


def one_hot(column, offset):
    place = lax.broadcasted_iota(jnp.int32, column.shape, column.ndim - 1)
    return jnp.where(column == place + offset, 1.0, 0.0).astype(BF)


def one_hot_rows(row, offset):
    place = lax.broadcasted_iota(jnp.int32, row.shape, 0)
    return jnp.where(row == place + offset, 1.0, 0.0).astype(BF)


def local_senders(row, where, half_grid):
    at = row - where[0] * (2 * half_grid) - where[1] * half_grid
    return jnp.where(at < 0, at + 2 * half_grid, at)


def local_receivers(row, slot, where, piece):
    at = row - (where[0] - 1) * (2 * piece)
    owner = jnp.where(at >= 2 * piece, 1, 0) + jnp.where(at >= 4 * piece, 1, 0)
    within = at - owner * (2 * piece)
    half = jnp.where(within >= piece, 1, 0)
    flip = jnp.where(half == where[1], 0, 1)
    place = jnp.where(where[0] % 2 == 0, 2 - owner, owner)
    near = (flip * 3 + place) * piece + within - half * piece
    return jnp.where(slot < where[2], near, -1)


def index_row(group, groups, where):
    at = group + where[1] * (groups // 2)
    return jnp.where(at >= groups, at - groups, at)


def copies(pairs, sems):
    return [pltpu.make_async_copy(src, dst, sems.at[k]) for k, (src, dst) in enumerate(pairs)]


def sender_kernel(
    band,
    chan,
    grid_own,
    grid_far,
    edge_own,
    edge_far,
    w_grid,
    w_edge,
    bias,
    senders,
    pre_out,
    grid,
    edge,
    pre,
    table,
    left,
    in_sems,
    out_sems,
):
    where = (band[0], chan[0])
    half_edges = edge_own.shape[0]
    half_grid = grid_own.shape[0]
    n_grid = 2 * half_grid
    block = left.shape[0]
    fetches = copies(
        (
            (grid_own, grid.at[0:half_grid]),
            (grid_far, grid.at[half_grid:]),
            (edge_own, edge.at[0:half_edges]),
            (edge_far, edge.at[half_edges:]),
        ),
        in_sems,
    )
    for f in fetches:
        f.start()
    table[n_grid:] = w_edge[...]
    fetches[0].wait()
    fetches[1].wait()
    table[0:n_grid] = dot(grid[...], w_grid[...]).astype(BF)
    fetches[2].wait()
    fetches[3].wait()
    groups = 2 * half_edges // LANES
    per = block // LANES
    steps = 2 * half_edges // block

    def step(i, carry):
        rows = pl.ds(pl.multiple_of(i * block, block), block)
        for c in range(per):
            at = index_row(i * per + c, groups, where)
            row = local_senders(senders[pl.ds(at, 1), :], where, half_grid)
            column = jnp.broadcast_to(row, (LANES, LANES)).T
            for k in range(n_grid // LANES):
                left[c * LANES : (c + 1) * LANES, k * LANES : (k + 1) * LANES] = one_hot(column, k * LANES)
        left[:, n_grid:] = edge[rows, :]
        pre[rows, :] = dot(left[...], table[...]) + bias[...]
        pltpu.make_async_copy(pre.at[rows], pre_out.at[rows], out_sems.at[i]).start()
        return carry

    lax.fori_loop(0, steps, step, 0)
    for k in range(steps):
        rows = pl.ds(k * block, block)
        pltpu.make_async_copy(pre.at[rows], pre_out.at[rows], out_sems.at[k]).wait()


def edge_kernel(
    band,
    chan,
    count,
    grid_own,
    grid_far,
    edge_own,
    edge_far,
    m0,
    m1,
    m2,
    m3,
    m4,
    m5,
    w_mesh,
    w_out,
    pre_in,
    senders,
    receivers,
    wire_out,
    cot_own,
    cot_far,
    seg_out,
    rim_low,
    rim_mid,
    rim_high,
    grid,
    edge,
    pre_part,
    lat,
    cot,
    table,
    left,
    right,
    sums,
    act_sums,
    edge_sum,
    bias_sum,
    cots,
    seg_grid,
    wire,
    low_v,
    mid_v,
    high_v,
    in_sems,
    out_sems,
):
    where = (band[0], chan[0], count[0])
    half_edges = edge_own.shape[0]
    half_grid = grid_own.shape[0]
    n_grid = 2 * half_grid
    piece = m0.shape[1]
    n_mesh = 6 * piece
    pad_mesh = lat.shape[0]
    n_rows = n_grid + pad_mesh
    block = left.shape[0]
    hidden = w_mesh.shape[1]
    pieces = (m0, m1, m2, m3, m4, m5)
    lats = [(m.at[0], lat.at[k * piece : (k + 1) * piece]) for k, m in enumerate(pieces)]
    cot_pairs = [(m.at[1], cot.at[k * piece : (k + 1) * piece]) for k, m in enumerate(pieces)]
    rest = [
        (pre_in, pre_part),
        (edge_own, edge.at[0:half_edges]),
        (edge_far, edge.at[half_edges:]),
        (grid_own, grid.at[0:half_grid]),
        (grid_far, grid.at[half_grid:]),
    ]
    fetches = copies(lats + cot_pairs + rest, in_sems)
    for f in fetches:
        f.start()
    if pad_mesh > n_mesh:
        lat[n_mesh:] = jnp.zeros((pad_mesh - n_mesh, lat.shape[1]), BF)
        cot[n_mesh:] = jnp.zeros((pad_mesh - n_mesh, cot.shape[1]), BF)
    sums[...] = jnp.zeros_like(sums)
    act_sums[...] = jnp.zeros_like(act_sums)
    edge_sum[...] = jnp.zeros_like(edge_sum)
    bias_sum[...] = jnp.zeros_like(bias_sum)
    for f in fetches[0:12]:
        f.wait()
    table[:, 0:hidden] = dot(lat[...], w_mesh[...]).astype(BF)
    cot_terms = dot_t(cot[...], w_out[...])
    high = cot_terms.astype(BF)
    table[:, hidden : 2 * hidden] = high
    table[:, 2 * hidden :] = (cot_terms - high.astype(F32)).astype(BF)
    for f in fetches[12:]:
        f.wait()
    groups = 2 * half_edges // LANES
    per = block // LANES

    def step(i, carry):
        rows = pl.ds(pl.multiple_of(i * block, block), block)
        for c in range(per):
            at = index_row(i * per + c, groups, where)
            mine = slice(c * LANES, (c + 1) * LANES)
            slot = at * LANES + lax.broadcasted_iota(jnp.int32, (1, LANES), 1)
            row = local_receivers(receivers[pl.ds(at, 1), :], slot, where, piece)
            row = jnp.broadcast_to(row, (LANES, LANES))
            column = row.T
            for k in range(pad_mesh // LANES):
                left[mine, k * LANES : (k + 1) * LANES] = one_hot(column, k * LANES)
                at_row = n_grid + k * LANES
                right[at_row : at_row + LANES, mine] = one_hot_rows(row, k * LANES)
            row = local_senders(senders[pl.ds(at, 1), :], where, half_grid)
            row = jnp.broadcast_to(row, (LANES, LANES))
            for k in range(n_grid // LANES):
                right[k * LANES : (k + 1) * LANES, mine] = one_hot_rows(row, k * LANES)
        got = dot(left[...], table[...])
        pre = pre_part[rows, :] + got[:, 0:hidden]
        hidden_cot = got[:, hidden : 2 * hidden] + got[:, 2 * hidden :]
        sig = jax.nn.sigmoid(pre)
        act = (pre * sig).astype(BF)
        pre_cot = (hidden_cot * sig * (1.0 + pre * (1.0 - sig))).astype(BF)
        cots[rows, :] = pre_cot
        sums[...] += dot(right[...], pre_cot)
        act_sums[...] += dot(right[n_grid:, :], act)
        edge_sum[...] += dot_rows(edge[rows, :], pre_cot)
        bias_sum[...] += pre_cot.astype(F32).reshape(block // 8, 8, hidden).sum(axis=0)
        return carry

    lax.fori_loop(0, 2 * half_edges // block, step, 0)

    seg_grid[...] = sums[:n_grid].astype(BF)
    for ref, o, kind in ((low_v, 0, BF), (mid_v, 1, F32), (high_v, 2, BF)):
        for h in range(2):
            start = n_grid + (3 * h + o) * piece
            ref[h * piece : (h + 1) * piece] = sums[start : start + piece].astype(kind)
    rows = ROWS
    per_grad = w_mesh.shape[0] // rows
    parts = [slice(k * per_grad, (k + 1) * per_grad) for k in range(4)]
    stores = copies(
        [
            (low_v, rim_low),
            (high_v, rim_high),
            (seg_grid, seg_out),
            (cots.at[0:half_edges], cot_own),
            (cots.at[half_edges:], cot_far),
            (mid_v, rim_mid),
        ]
        + [(wire.at[p, 0 : 2 * ROWS + TAIL], wire_out.at[p]) for p in parts],
        out_sems,
    )
    for f in stores[0:6]:
        f.start()
    sub = lax.broadcasted_iota(jnp.int32, (16, LANES), 0)
    bias_total = jnp.sum(bias_sum[...], axis=0, keepdims=True)
    low = jnp.broadcast_to(bias_total[:, :LANES], (16, LANES))
    high = jnp.broadcast_to(bias_total[:, LANES:], (16, LANES))
    tail = jnp.where(sub == 0, low, jnp.where(sub == 1, high, 0.0)).astype(BF)
    for k in range(wire.shape[0]):
        wire[k, 2 * rows :, :] = tail

    def put_all(at, g):
        for k in range(g.shape[0] // rows):
            value = g[k * rows : (k + 1) * rows]
            wire[at + k, 0:rows, :] = value[:, :LANES].astype(BF)
            wire[at + k, rows : 2 * rows, :] = value[:, LANES:].astype(BF)

    put_all(parts[2].start, edge_sum[...])
    stores[8].start()
    put_all(parts[0].start, dot_rows(grid[...], seg_grid[...]))
    stores[6].start()
    put_all(parts[1].start, dot_rows(lat[...], sums[n_grid:].astype(BF)))
    stores[7].start()
    g = dot_rows(act_sums[...].astype(BF), cot[...])
    put_all(parts[3].start, g[:, 0:hidden])
    put_all(parts[3].start + per_grad // 2, g[:, hidden:])
    stores[9].start()
    for f in stores:
        f.wait()


def swap(x):
    return lax.ppermute(x, "chan", [(0, 1), (1, 0)])


def pair_swap(x, first):
    n = lax.axis_size(BAND)
    pairs = [(i, i + 1) for i in range(first, n - 1, 2)]
    return lax.ppermute(x, BAND, pairs + [(j, i) for i, j in pairs])


def depth_total(mine):
    depth = lax.axis_size("zh")
    step = 1
    while True:
        mask = depth - 1 if 2 * step == depth else step
        other = lax.ppermute(mine, "zh", [(i, i ^ mask) for i in range(depth)])
        total = mine.astype(F32) + other.astype(F32)
        step *= 2
        if step == depth:
            return total
        mine = total.astype(BF)


def body(
    grid_latent,
    edge_latent,
    mesh_latent,
    mesh_cotangent,
    w_grid,
    w_mesh,
    w_edge,
    bias,
    w_out,
    senders,
    receivers,
    edge_count,
):
    band = lax.axis_index(BAND)
    chan = lax.axis_index("chan")
    half_grid = grid_latent.shape[0]
    half_edges = edge_latent.shape[0]
    piece, width = mesh_latent.shape
    hidden = w_grid.shape[1]
    n_grid = 2 * half_grid
    pad_mesh = -(-6 * piece // LANES) * LANES

    mesh_own = jnp.stack([mesh_latent, mesh_cotangent])
    mesh_low = pair_swap(mesh_own, 0)
    mesh_high = pair_swap(mesh_own, 1)
    edge_far = swap(edge_latent)
    grid_far = swap(grid_latent)
    mesh_own_far = swap(mesh_own)

    senders = senders.reshape(-1, LANES)
    receivers = receivers.reshape(-1, LANES)
    shape = jax.ShapeDtypeStruct
    vmem = pl.BlockSpec(memory_space=pltpu.VMEM)
    smem = pl.BlockSpec(memory_space=pltpu.SMEM)
    params = pltpu.CompilerParams(vmem_limit_bytes=56 * 1024 * 1024)
    anywhere = pl.BlockSpec(memory_space=pl.ANY)
    dma = pltpu.SemaphoreType.DMA
    n_edges = 2 * half_edges
    pre = pl.pallas_call(
        sender_kernel,
        out_shape=shape((n_edges, hidden), F32),
        in_specs=[smem] * 2 + [anywhere] * 4 + [vmem] * 4,
        out_specs=anywhere,
        scratch_shapes=[
            pltpu.VMEM((n_grid, width), BF),
            pltpu.VMEM((n_edges, width), BF),
            pltpu.VMEM((n_edges, hidden), F32),
            pltpu.VMEM((n_grid + width, hidden), BF),
            pltpu.VMEM((EDGE_BLOCK, n_grid + width), BF),
            dma((4,)),
            dma((n_edges // EDGE_BLOCK,)),
        ],
        compiler_params=params,
        cost_estimate=pl.CostEstimate(flops=SENDER_FLOPS, transcendentals=0, bytes_accessed=1 << 22),
        name="sender_step",
    )(band.reshape(1), chan.reshape(1), grid_latent, grid_far, edge_latent, edge_far, w_grid, w_edge, bias.reshape(1, hidden), senders)

    mesh_low, mesh_high, pre = lax.optimization_barrier((mesh_low, mesh_high, pre))
    mesh_near = (mesh_low, mesh_own, mesh_high)
    mesh_far = (swap(mesh_low), mesh_own_far, swap(mesh_high))
    wire, cot_own, cot_far, seg_grid, rim_low, rim_mid, rim_high = pl.pallas_call(
        edge_kernel,
        out_shape=(
            shape((MEMBERS, 2 * ROWS + TAIL, LANES), BF),
            shape((half_edges, hidden), BF),
            shape((half_edges, hidden), BF),
            shape((n_grid, hidden), BF),
            shape((2 * piece, hidden), BF),
            shape((2 * piece, hidden), F32),
            shape((2 * piece, hidden), BF),
        ),
        in_specs=[smem] * 3 + [anywhere] * 10 + [vmem] * 2 + [anywhere] + [vmem] * 2,
        out_specs=(anywhere,) * 7,
        scratch_shapes=[
            pltpu.VMEM((n_grid, width), BF),
            pltpu.VMEM((n_edges, width), BF),
            pltpu.VMEM((n_edges, hidden), F32),
            pltpu.VMEM((pad_mesh, width), BF),
            pltpu.VMEM((pad_mesh, width), BF),
            pltpu.VMEM((pad_mesh, 3 * hidden), BF),
            pltpu.VMEM((EDGE_BLOCK, pad_mesh), BF),
            pltpu.VMEM((n_grid + pad_mesh, EDGE_BLOCK), BF),
            pltpu.VMEM((n_grid + pad_mesh, hidden), F32),
            pltpu.VMEM((pad_mesh, hidden), F32),
            pltpu.VMEM((width, hidden), F32),
            pltpu.VMEM((8, hidden), F32),
            pltpu.VMEM((n_edges, hidden), BF),
            pltpu.VMEM((n_grid, hidden), BF),
            pltpu.VMEM((MEMBERS, 2 * ROWS + 16, LANES), BF),
            pltpu.VMEM((2 * piece, hidden), BF),
            pltpu.VMEM((2 * piece, hidden), F32),
            pltpu.VMEM((2 * piece, hidden), BF),
            dma((17,)),
            dma((10,)),
        ],
        compiler_params=params,
        cost_estimate=pl.CostEstimate(flops=EDGE_FLOPS, transcendentals=1 << 20, bytes_accessed=1 << 23),
        name="edge_step",
    )(
        band.reshape(1),
        chan.reshape(1),
        edge_count,
        grid_latent,
        grid_far,
        edge_latent,
        edge_far,
        *mesh_near,
        *mesh_far,
        w_mesh,
        w_out,
        pre,
        senders,
        receivers,
    )

    from_low = pair_swap(rim_low, 0)
    from_high = pair_swap(rim_high, 1)
    arrived = lax.all_to_all(wire, GROUP, 0, 0, tiled=True)
    edge_term = dot_t(cot_far, w_edge).astype(BF)
    grid_term = dot_t(seg_grid[half_grid:], w_grid).astype(BF)
    edge_back = swap(edge_term)
    grid_back = swap(grid_term)
    total = arrived.astype(F32).sum(axis=0).astype(BF)
    total, from_low, from_high, _, _ = lax.optimization_barrier((total, from_low, from_high, edge_term, grid_term))
    total = depth_total(total)
    grad_bias = total[2 * ROWS : 2 * ROWS + 2].reshape(hidden)
    chunk = jnp.concatenate([total[:ROWS], total[ROWS : 2 * ROWS]], axis=1).astype(BF)
    spread = jnp.broadcast_to(chunk[None], (MEMBERS, ROWS, hidden))
    everyone = lax.all_to_all(spread, GROUP, 0, 0, tiled=True)

    grad_edge = (dot_t(cot_own, w_edge) + edge_back.astype(F32)).astype(BF)
    grad_grid = (dot_t(seg_grid[:half_grid], w_grid) + grid_back.astype(F32)).astype(BF)
    seg_mesh = (rim_mid + from_low.astype(F32) + from_high.astype(F32)).astype(BF)
    seg_mesh, _ = lax.optimization_barrier((seg_mesh, chunk))
    mesh_back = swap(dot_t(seg_mesh[piece:], w_mesh).astype(BF))
    grad_mesh = (dot_t(seg_mesh[:piece], w_mesh) + mesh_back.astype(F32)).astype(BF)

    def rows_of(start, stop):
        return everyone[start:stop].astype(F32).reshape(-1, hidden)

    q = MEMBERS // 4
    return (
        grad_grid,
        grad_edge,
        grad_mesh,
        rows_of(0, q),
        rows_of(q, 2 * q),
        rows_of(2 * q, 3 * q),
        grad_bias,
        jnp.concatenate([rows_of(3 * q, 3 * q + q // 2), rows_of(3 * q + q // 2, 4 * q)], axis=1),
    )


def solution(mesh):
    bands, chans = (mesh.shape["band"], mesh.shape["chan"])
    side = 4
    inner = Mesh(np.asarray(mesh.devices).reshape(bands // (2 * side**2), 2, side, side, chans), (*BAND, "chan"))
    every = P((*BAND, "chan"), None)
    return jax.shard_map(
        body,
        mesh=inner,
        in_specs=(
            every,
            every,
            every,
            every,
            P(None, "chan"),
            P(None, "chan"),
            P(None, "chan"),
            P("chan"),
            P("chan", None),
            P(BAND),
            P(BAND),
            P(BAND),
        ),
        out_specs=(
            every,
            every,
            every,
            P(None, "chan"),
            P(None, "chan"),
            P(None, "chan"),
            P("chan"),
            P("chan", None),
        ),
        check_vma=False,
    )
```

```python
import functools

import jax
import jax.numpy as jnp
import numpy as np
from jax import lax
from jax.experimental import pallas as pl
from jax.experimental.pallas import tpu as pltpu
from jax.sharding import Mesh, PartitionSpec as P

BF = jnp.bfloat16
F32 = jnp.float32
BAND = ("zh", "zl", "y", "x")
GROUP = ("zl", "y", "x")
LANES = 128
EDGE_BLOCK = 768
UNIT = 384
TAIL = 8
ROWS = 64
MEMBERS = 32
SENDER_FLOPS = 4 * 10**9
EDGE_FLOPS = 9 * 10**9


def dot(a, b):
    return jnp.dot(a, b, preferred_element_type=F32)


def dot_t(a, b):
    return lax.dot_general(a, b, (((1,), (1,)), ((), ())), preferred_element_type=F32)


def dot_rows(a, b):
    return lax.dot_general(a, b, (((0,), (0,)), ((), ())), preferred_element_type=F32)


def one_hot(column, offset):
    place = lax.broadcasted_iota(jnp.int32, column.shape, column.ndim - 1)
    return jnp.where(column == place + offset, 1.0, 0.0).astype(BF)


def one_hot_rows(row, offset):
    place = lax.broadcasted_iota(jnp.int32, row.shape, 0)
    return jnp.where(row == place + offset, 1.0, 0.0).astype(BF)


def local_senders(row, where, half_grid):
    at = row - where[0] * (2 * half_grid) - where[1] * half_grid
    return jnp.where(at < 0, at + 2 * half_grid, at)


def local_receivers(row, slot, where, piece):
    at = row - (where[0] - 1) * (2 * piece)
    owner = jnp.where(at >= 2 * piece, 1, 0) + jnp.where(at >= 4 * piece, 1, 0)
    within = at - owner * (2 * piece)
    half = jnp.where(within >= piece, 1, 0)
    flip = jnp.where(half == where[1], 0, 1)
    place = jnp.where(where[0] % 2 == 0, 2 - owner, owner)
    near = (flip * 3 + place) * piece + within - half * piece
    return jnp.where(slot < where[2], near, -1)


def index_row(group, groups, where):
    at = group + where[1] * (groups // 2)
    return jnp.where(at >= groups, at - groups, at)


def copies(pairs, sems):
    return [pltpu.make_async_copy(src, dst, sems.at[k]) for k, (src, dst) in enumerate(pairs)]


def sender_kernel(
    band,
    chan,
    grid_own,
    grid_far,
    edge_own,
    edge_far,
    w_grid,
    w_edge,
    bias,
    senders,
    pre,
    grid,
    edge,
    table,
    left,
    in_sems,
):
    where = (band[0], chan[0])
    half_edges = edge_own.shape[0]
    half_grid = grid_own.shape[0]
    n_grid = 2 * half_grid
    block = left.shape[0]
    fetches = copies(((grid_own, grid), (edge_own, edge)), in_sems)
    for f in fetches:
        f.start()
    table[n_grid:] = w_edge[...]
    table[half_grid:n_grid] = dot(grid_far[...], w_grid[...]).astype(BF)
    fetches[0].wait()
    table[0:half_grid] = dot(grid[...], w_grid[...]).astype(BF)
    fetches[1].wait()
    groups = 2 * half_edges // LANES
    per = block // LANES
    units = block // UNIT
    near = half_edges // UNIT

    def step(i, carry):
        rows = pl.ds(pl.multiple_of(i * block, block), block)
        for h in range(units):
            at = i * units + h
            mine = slice(h * UNIT, (h + 1) * UNIT)

            @pl.when(at < near)
            def _():
                left[mine, n_grid:] = edge[pl.ds(pl.multiple_of(at * UNIT, UNIT), UNIT), :]

            @pl.when(at >= near)
            def _():
                left[mine, n_grid:] = edge_far[pl.ds(pl.multiple_of((at - near) * UNIT, UNIT), UNIT), :]

        for c in range(per):
            at = index_row(i * per + c, groups, where)
            row = local_senders(senders[pl.ds(at, 1), :], where, half_grid)
            column = jnp.broadcast_to(row, (LANES, LANES)).T
            for k in range(n_grid // LANES):
                left[c * LANES : (c + 1) * LANES, k * LANES : (k + 1) * LANES] = one_hot(column, k * LANES)
        pre[rows, :] = dot(left[...], table[...]) + bias[...]
        return carry

    lax.fori_loop(0, 2 * half_edges // block, step, 0)


def edge_kernel(
    band,
    chan,
    count,
    grid_own,
    grid_far,
    edge_own,
    edge_far,
    m0,
    m1,
    m2,
    m3,
    m4,
    m5,
    w_mesh,
    w_out,
    pre_part,
    senders,
    receivers,
    wire_out,
    cots,
    seg_grid,
    rim_low,
    rim_mid,
    rim_high,
    grid,
    edge,
    lat,
    cot,
    table,
    left,
    right,
    sums,
    act_sums,
    edge_sum,
    bias_sum,
    wire,
    low_v,
    high_v,
    in_sems,
    edge_sems,
    out_sems,
):
    where = (band[0], chan[0], count[0])
    half_edges = edge_own.shape[0]
    half_grid = grid_own.shape[0]
    n_grid = 2 * half_grid
    piece = m0.shape[1]
    n_mesh = 6 * piece
    pad_mesh = lat.shape[0]
    n_rows = n_grid + pad_mesh
    block = left.shape[0]
    hidden = w_mesh.shape[1]
    near = half_edges // UNIT
    apart = ((0, m0), (1, m1), (2, m2), (4, m4))
    lats = [(m.at[0], lat.at[k * piece : (k + 1) * piece]) for k, m in apart]
    cot_pairs = [(m.at[1], cot.at[k * piece : (k + 1) * piece]) for k, m in apart]
    grids = [(grid_own, grid.at[0:half_grid]), (grid_far, grid.at[half_grid:])]
    fetches = copies(lats + cot_pairs + grids, in_sems)
    edges = [
        (source.at[k * UNIT : (k + 1) * UNIT], edge.at[(k + off) * UNIT : (k + off + 1) * UNIT])
        for source, off in ((edge_own, 0), (edge_far, near))
        for k in range(near)
    ]
    for f in fetches[0:8] + copies(edges, edge_sems) + fetches[8:]:
        f.start()
    for k, m in ((3, m3), (5, m5)):
        lat[k * piece : (k + 1) * piece] = m[0]
        cot[k * piece : (k + 1) * piece] = m[1]
    if pad_mesh > n_mesh:
        lat[n_mesh:] = jnp.zeros((pad_mesh - n_mesh, lat.shape[1]), BF)
        cot[n_mesh:] = jnp.zeros((pad_mesh - n_mesh, cot.shape[1]), BF)
    sums[...] = jnp.zeros_like(sums)
    act_sums[...] = jnp.zeros_like(act_sums)
    edge_sum[...] = jnp.zeros_like(edge_sum)
    bias_sum[...] = jnp.zeros_like(bias_sum)
    for f in fetches[0:8]:
        f.wait()
    table[:, 0:hidden] = dot(lat[...], w_mesh[...]).astype(BF)
    cot_terms = dot_t(cot[...], w_out[...])
    high = cot_terms.astype(BF)
    table[:, hidden : 2 * hidden] = high
    table[:, 2 * hidden :] = (cot_terms - high.astype(F32)).astype(BF)
    groups = 2 * half_edges // LANES
    per = block // LANES

    def step(i, carry):
        rows = pl.ds(pl.multiple_of(i * block, block), block)
        for c in range(per):
            at = index_row(i * per + c, groups, where)
            mine = slice(c * LANES, (c + 1) * LANES)
            slot = at * LANES + lax.broadcasted_iota(jnp.int32, (1, LANES), 1)
            row = local_receivers(receivers[pl.ds(at, 1), :], slot, where, piece)
            row = jnp.broadcast_to(row, (LANES, LANES))
            column = row.T
            for k in range(pad_mesh // LANES):
                left[mine, k * LANES : (k + 1) * LANES] = one_hot(column, k * LANES)
                at_row = n_grid + k * LANES
                right[at_row : at_row + LANES, mine] = one_hot_rows(row, k * LANES)
            row = local_senders(senders[pl.ds(at, 1), :], where, half_grid)
            row = jnp.broadcast_to(row, (LANES, LANES))
            for k in range(n_grid // LANES):
                right[k * LANES : (k + 1) * LANES, mine] = one_hot_rows(row, k * LANES)
        got = dot(left[...], table[...])
        pre = pre_part[rows, :] + got[:, 0:hidden]
        hidden_cot = got[:, hidden : 2 * hidden] + got[:, 2 * hidden :]
        sig = jax.nn.sigmoid(pre)
        act = (pre * sig).astype(BF)
        pre_cot = (hidden_cot * sig * (1.0 + pre * (1.0 - sig))).astype(BF)
        cots[rows, :] = pre_cot
        sums[...] += dot(right[...], pre_cot)
        act_sums[...] += dot(right[n_grid:, :], act)
        for h in range(block // UNIT):
            at = i * (block // UNIT) + h
            unit = pl.ds(pl.multiple_of(at * UNIT, UNIT), UNIT)
            pltpu.make_async_copy(edge_own.at[0:UNIT], edge.at[unit], edge_sems.at[at]).wait()
        edge_sum[...] += dot_rows(edge[rows, :], pre_cot)
        bias_sum[...] += pre_cot.astype(F32).reshape(block // 8, 8, hidden).sum(axis=0)
        return carry

    lax.fori_loop(0, 2 * half_edges // block, step, 0)

    seg_grid[...] = sums[:n_grid].astype(BF)
    for ref, o, kind in ((low_v, 0, BF), (rim_mid, 1, F32), (high_v, 2, BF)):
        for h in range(2):
            start = n_grid + (3 * h + o) * piece
            ref[h * piece : (h + 1) * piece] = sums[start : start + piece].astype(kind)
    rows = ROWS
    per_grad = w_mesh.shape[0] // rows
    parts = [slice(k * per_grad, (k + 1) * per_grad) for k in range(4)]
    stores = copies(
        [(low_v, rim_low), (high_v, rim_high)] + [(wire.at[p, 0 : 2 * ROWS + TAIL], wire_out.at[p]) for p in parts],
        out_sems,
    )
    for f in stores[0:2]:
        f.start()
    for f in fetches[8:]:
        f.wait()
    sub = lax.broadcasted_iota(jnp.int32, (16, LANES), 0)
    bias_total = jnp.sum(bias_sum[...], axis=0, keepdims=True)
    low = jnp.broadcast_to(bias_total[:, :LANES], (16, LANES))
    high = jnp.broadcast_to(bias_total[:, LANES:], (16, LANES))
    tail = jnp.where(sub == 0, low, jnp.where(sub == 1, high, 0.0)).astype(BF)
    for k in range(wire.shape[0]):
        wire[k, 2 * rows :, :] = tail

    def put_all(at, g):
        for k in range(g.shape[0] // rows):
            value = g[k * rows : (k + 1) * rows]
            wire[at + k, 0:rows, :] = value[:, :LANES].astype(BF)
            wire[at + k, rows : 2 * rows, :] = value[:, LANES:].astype(BF)

    put_all(parts[2].start, edge_sum[...])
    stores[4].start()
    put_all(parts[0].start, dot_rows(grid[...], seg_grid[...]))
    stores[2].start()
    put_all(parts[1].start, dot_rows(lat[...], sums[n_grid:].astype(BF)))
    stores[3].start()
    g = dot_rows(act_sums[...].astype(BF), cot[...])
    put_all(parts[3].start, g[:, 0:hidden])
    put_all(parts[3].start + per_grad // 2, g[:, hidden:])
    stores[5].start()
    for f in stores:
        f.wait()


def swap(x):
    return lax.ppermute(x, "chan", [(0, 1), (1, 0)])


def pair_swap(x, first):
    n = lax.axis_size(BAND)
    pairs = [(i, i + 1) for i in range(first, n - 1, 2)]
    return lax.ppermute(x, BAND, pairs + [(j, i) for i, j in pairs])


def depth_total(mine):
    depth = lax.axis_size("zh")
    step = 1
    while True:
        mask = depth - 1 if 2 * step == depth else step
        other = lax.ppermute(mine, "zh", [(i, i ^ mask) for i in range(depth)])
        total = mine.astype(F32) + other.astype(F32)
        step *= 2
        if step == depth:
            return total
        mine = total.astype(BF)


def body(
    grid_latent,
    edge_latent,
    mesh_latent,
    mesh_cotangent,
    w_grid,
    w_mesh,
    w_edge,
    bias,
    w_out,
    senders,
    receivers,
    edge_count,
):
    band = lax.axis_index(BAND)
    chan = lax.axis_index("chan")
    half_grid = grid_latent.shape[0]
    half_edges = edge_latent.shape[0]
    piece, width = mesh_latent.shape
    hidden = w_grid.shape[1]
    n_grid = 2 * half_grid
    pad_mesh = -(-6 * piece // LANES) * LANES

    mesh_own = jnp.stack([mesh_latent, mesh_cotangent])
    mesh_low = pair_swap(mesh_own, 0)
    mesh_high = pair_swap(mesh_own, 1)
    edge_far = swap(edge_latent)
    grid_far = swap(grid_latent)
    mesh_own_far = swap(mesh_own)

    senders = senders.reshape(-1, LANES)
    receivers = receivers.reshape(-1, LANES)
    vmem = pl.BlockSpec(memory_space=pltpu.VMEM)
    smem = pl.BlockSpec(memory_space=pltpu.SMEM)
    small, large = [pltpu.CompilerParams(vmem_limit_bytes=n * 2**20) for n in (16, 32)]

    def near(x):
        return pltpu.with_memory_space_constraint(x, pltpu.VMEM)

    def wide(*arrays):
        return [pltpu.with_memory_space_constraint(x, pltpu.HBM) for x in arrays]

    def scalars(*arrays):
        return [pltpu.with_memory_space_constraint(x, pltpu.SMEM) for x in arrays]

    anywhere = pl.BlockSpec(memory_space=pl.ANY)
    dma = pltpu.SemaphoreType.DMA
    n_edges = 2 * half_edges
    pre = pl.pallas_call(
        sender_kernel,
        out_shape=pltpu.VMEM((n_edges, hidden), F32),
        in_specs=[smem] * 2 + [anywhere, vmem] * 2 + [vmem] * 4,
        out_specs=vmem,
        scratch_shapes=[
            pltpu.VMEM((half_grid, width), BF),
            pltpu.VMEM((half_edges, width), BF),
            pltpu.VMEM((n_grid + width, hidden), BF),
            pltpu.VMEM((EDGE_BLOCK, n_grid + width), BF),
            dma((2,)),
        ],
        compiler_params=small,
        cost_estimate=pl.CostEstimate(flops=SENDER_FLOPS, transcendentals=0, bytes_accessed=1 << 22),
        name="sender_step",
    )(
        *scalars(band.reshape(1), chan.reshape(1)),
        *wide(grid_latent),
        near(grid_far),
        *wide(edge_latent),
        near(edge_far),
        *wide(w_grid, w_edge, bias.reshape(1, hidden), senders),
    )

    mesh_low, mesh_high, pre = lax.optimization_barrier((mesh_low, mesh_high, pre))
    mesh_near = (mesh_low, mesh_own, mesh_high)
    mesh_far = [near(swap(mesh_low)), *wide(mesh_own_far), near(swap(mesh_high))]
    wire, cots, seg_grid, rim_low, rim_mid, rim_high = pl.pallas_call(
        edge_kernel,
        out_shape=(
            pltpu.HBM((MEMBERS, 2 * ROWS + TAIL, LANES), BF),
            pltpu.VMEM((n_edges, hidden), BF),
            pltpu.VMEM((n_grid, hidden), BF),
            pltpu.HBM((2 * piece, hidden), BF),
            pltpu.VMEM((2 * piece, hidden), F32),
            pltpu.HBM((2 * piece, hidden), BF),
        ),
        in_specs=[smem] * 3 + [anywhere] * 7 + [vmem] * 8,
        out_specs=(anywhere, vmem, vmem, anywhere, vmem, anywhere),
        scratch_shapes=[
            pltpu.VMEM((n_grid, width), BF),
            pltpu.VMEM((n_edges, width), BF),
            pltpu.VMEM((pad_mesh, width), BF),
            pltpu.VMEM((pad_mesh, width), BF),
            pltpu.VMEM((pad_mesh, 3 * hidden), BF),
            pltpu.VMEM((EDGE_BLOCK, pad_mesh), BF),
            pltpu.VMEM((n_grid + pad_mesh, EDGE_BLOCK), BF),
            pltpu.VMEM((n_grid + pad_mesh, hidden), F32),
            pltpu.VMEM((pad_mesh, hidden), F32),
            pltpu.VMEM((width, hidden), F32),
            pltpu.VMEM((8, hidden), F32),
            pltpu.VMEM((MEMBERS, 2 * ROWS + 16, LANES), BF),
            pltpu.VMEM((2 * piece, hidden), BF),
            pltpu.VMEM((2 * piece, hidden), BF),
            dma((10,)),
            dma((n_edges // UNIT,)),
            dma((6,)),
        ],
        compiler_params=large,
        cost_estimate=pl.CostEstimate(flops=EDGE_FLOPS, transcendentals=1 << 20, bytes_accessed=1 << 23),
        name="edge_step",
    )(
        *scalars(band.reshape(1), chan.reshape(1), edge_count),
        *wide(grid_latent, grid_far, edge_latent, edge_far, *mesh_near),
        *mesh_far,
        *wide(w_mesh, w_out),
        near(pre),
        *wide(senders, receivers),
    )

    cot_own, cot_far = (cots[:half_edges], cots[half_edges:])
    from_low = pair_swap(rim_low, 0)
    from_high = pair_swap(rim_high, 1)
    arrived = lax.all_to_all(wire, GROUP, 0, 0, tiled=True)
    edge_term = dot_t(cot_far, w_edge).astype(BF)
    grid_term = dot_t(seg_grid[half_grid:], w_grid).astype(BF)
    edge_back = swap(edge_term)
    grid_back = swap(grid_term)
    total = arrived.astype(F32).sum(axis=0).astype(BF)
    total, from_low, from_high, _, _ = lax.optimization_barrier((total, from_low, from_high, edge_term, grid_term))
    total = depth_total(total)
    grad_bias = total[2 * ROWS : 2 * ROWS + 2].reshape(hidden)
    chunk = jnp.concatenate([total[:ROWS], total[ROWS : 2 * ROWS]], axis=1).astype(BF)
    spread = jnp.broadcast_to(chunk[None], (MEMBERS, ROWS, hidden))
    everyone = lax.all_to_all(spread, GROUP, 0, 0, tiled=True)

    grad_edge = (dot_t(cot_own, w_edge) + edge_back.astype(F32)).astype(BF)
    grad_grid = (dot_t(seg_grid[:half_grid], w_grid) + grid_back.astype(F32)).astype(BF)
    seg_mesh = (rim_mid + from_low.astype(F32) + from_high.astype(F32)).astype(BF)
    seg_mesh, _ = lax.optimization_barrier((seg_mesh, chunk))
    mesh_back = swap(dot_t(seg_mesh[piece:], w_mesh).astype(BF))
    grad_mesh = (dot_t(seg_mesh[:piece], w_mesh) + mesh_back.astype(F32)).astype(BF)

    def rows_of(start, stop):
        return everyone[start:stop].astype(F32).reshape(-1, hidden)

    q = MEMBERS // 4
    return (
        grad_grid,
        grad_edge,
        grad_mesh,
        rows_of(0, q),
        rows_of(q, 2 * q),
        rows_of(2 * q, 3 * q),
        grad_bias,
        jnp.concatenate([rows_of(3 * q, 3 * q + q // 2), rows_of(3 * q + q // 2, 4 * q)], axis=1),
    )


def solution(mesh):
    bands, chans = (mesh.shape["band"], mesh.shape["chan"])
    side = 4
    inner = Mesh(np.asarray(mesh.devices).reshape(bands // (2 * side**2), 2, side, side, chans), (*BAND, "chan"))
    every = P((*BAND, "chan"), None)
    return jax.shard_map(
        body,
        mesh=inner,
        in_specs=(
            every,
            every,
            every,
            every,
            P(None, "chan"),
            P(None, "chan"),
            P(None, "chan"),
            P("chan"),
            P("chan", None),
            P(BAND),
            P(BAND),
            P(BAND),
        ),
        out_specs=(
            every,
            every,
            every,
            P(None, "chan"),
            P(None, "chan"),
            P(None, "chan"),
            P("chan"),
            P("chan", None),
        ),
        check_vma=False,
    )
```

```python
import functools

import jax
import jax.numpy as jnp
import numpy as np
from jax import lax
from jax.experimental import pallas as pl
from jax.experimental.pallas import tpu as pltpu
from jax.sharding import Mesh, PartitionSpec as P

BF = jnp.bfloat16
F32 = jnp.float32
BAND = ("zh", "zl", "y", "x")
GROUP = ("zl", "y", "x")
LANES = 128
EDGE_BLOCK = 768
UNIT = 384
TAIL = 8
ROWS = 64
MEMBERS = 32
SENDER_FLOPS = 4 * 10**9
EDGE_FLOPS = 9 * 10**9


def dot(a, b):
    return jnp.dot(a, b, preferred_element_type=F32)


def dot_t(a, b):
    return lax.dot_general(a, b, (((1,), (1,)), ((), ())), preferred_element_type=F32)


def dot_rows(a, b):
    return lax.dot_general(a, b, (((0,), (0,)), ((), ())), preferred_element_type=F32)


def one_hot(column, offset):
    place = lax.broadcasted_iota(jnp.int32, column.shape, column.ndim - 1)
    return jnp.where(column == place + offset, 1.0, 0.0).astype(BF)


def one_hot_rows(row, offset):
    place = lax.broadcasted_iota(jnp.int32, row.shape, 0)
    return jnp.where(row == place + offset, 1.0, 0.0).astype(BF)


def local_senders(row, where, half_grid):
    at = row - where[0] * (2 * half_grid) - where[1] * half_grid
    return jnp.where(at < 0, at + 2 * half_grid, at)


def local_receivers(row, slot, where, piece):
    at = row - (where[0] - 1) * (2 * piece)
    owner = jnp.where(at >= 2 * piece, 1, 0) + jnp.where(at >= 4 * piece, 1, 0)
    within = at - owner * (2 * piece)
    half = jnp.where(within >= piece, 1, 0)
    flip = jnp.where(half == where[1], 0, 1)
    place = jnp.where(where[0] % 2 == 0, 2 - owner, owner)
    near = (flip * 3 + place) * piece + within - half * piece
    return jnp.where(slot < where[2], near, -1)


def index_row(group, groups, where):
    at = group + where[1] * (groups // 2)
    return jnp.where(at >= groups, at - groups, at)


def copies(pairs, sems):
    return [pltpu.make_async_copy(src, dst, sems.at[k]) for k, (src, dst) in enumerate(pairs)]


def sender_kernel(
    band,
    chan,
    grid_own,
    grid_far,
    edge_own,
    edge_far,
    w_grid,
    w_edge,
    bias_in,
    send_in,
    pre,
    grid,
    edge,
    weights,
    bias_row,
    senders,
    table,
    left,
    in_sems,
):
    where = (band[0], chan[0])
    half_edges = edge_own.shape[0]
    half_grid = grid_own.shape[0]
    n_grid = 2 * half_grid
    block = left.shape[0]
    fetches = copies(
        (
            (w_grid, weights),
            (grid_own, grid),
            (send_in, senders),
            (w_edge, table.at[n_grid:]),
            (bias_in, bias_row),
            (edge_own, edge),
        ),
        in_sems,
    )
    for f in fetches:
        f.start()
    fetches[0].wait()
    table[half_grid:n_grid] = dot(grid_far[...], weights[...]).astype(BF)
    fetches[1].wait()
    table[0:half_grid] = dot(grid[...], weights[...]).astype(BF)
    for f in fetches[2:]:
        f.wait()
    groups = 2 * half_edges // LANES
    per = block // LANES
    units = block // UNIT
    near = half_edges // UNIT

    def step(i, carry):
        rows = pl.ds(pl.multiple_of(i * block, block), block)
        for h in range(units):
            at = i * units + h
            mine = slice(h * UNIT, (h + 1) * UNIT)

            @pl.when(at < near)
            def _():
                left[mine, n_grid:] = edge[pl.ds(pl.multiple_of(at * UNIT, UNIT), UNIT), :]

            @pl.when(at >= near)
            def _():
                left[mine, n_grid:] = edge_far[pl.ds(pl.multiple_of((at - near) * UNIT, UNIT), UNIT), :]

        for c in range(per):
            at = index_row(i * per + c, groups, where)
            row = local_senders(senders[pl.ds(at, 1), :], where, half_grid)
            column = jnp.broadcast_to(row, (LANES, LANES)).T
            for k in range(n_grid // LANES):
                left[c * LANES : (c + 1) * LANES, k * LANES : (k + 1) * LANES] = one_hot(column, k * LANES)
        pre[rows, :] = dot(left[...], table[...]) + bias_row[...]
        return carry

    lax.fori_loop(0, 2 * half_edges // block, step, 0)


def edge_kernel(
    band,
    chan,
    count,
    grid_own,
    grid_far,
    edge_own,
    edge_far,
    m0,
    m1,
    m2,
    m3,
    m4,
    m5,
    w_mesh_in,
    w_out_in,
    pre_part,
    send_in,
    recv_in,
    wire_out,
    cots,
    seg_grid,
    rim_low,
    rim_mid,
    rim_high,
    grid,
    edge,
    lat,
    cot,
    table,
    left,
    right,
    both,
    sums,
    w_mesh,
    w_out,
    senders,
    receivers,
    wire,
    low_v,
    high_v,
    in_sems,
    edge_sems,
    out_sems,
):
    where = (band[0], chan[0], count[0])
    half_edges = edge_own.shape[0]
    half_grid = grid_own.shape[0]
    n_grid = 2 * half_grid
    piece = m0.shape[1]
    n_mesh = 6 * piece
    pad_mesh = lat.shape[0]
    n_rows = n_grid + pad_mesh
    block = left.shape[0]
    hidden = w_mesh.shape[1]
    near = half_edges // UNIT
    apart = ((0, m0), (1, m1), (2, m2), (4, m4))
    lats = [(m.at[0], lat.at[k * piece : (k + 1) * piece]) for k, m in apart]
    cot_pairs = [(m.at[1], cot.at[k * piece : (k + 1) * piece]) for k, m in apart]
    grids = [(grid_own, grid.at[0:half_grid]), (grid_far, grid.at[half_grid:])]
    small = [(w_mesh_in, w_mesh), (w_out_in, w_out), (send_in, senders), (recv_in, receivers)]
    fetches = copies(small + lats + cot_pairs + grids, in_sems)
    edges = [
        (source.at[k * UNIT : (k + 1) * UNIT], edge.at[(k + off) * UNIT : (k + off + 1) * UNIT])
        for source, off in ((edge_own, 0), (edge_far, near))
        for k in range(near)
    ]
    for f in fetches[0:12] + copies(edges, edge_sems) + fetches[12:]:
        f.start()
    for k, m in ((3, m3), (5, m5)):
        lat[k * piece : (k + 1) * piece] = m[0]
        cot[k * piece : (k + 1) * piece] = m[1]
    if pad_mesh > n_mesh:
        lat[n_mesh:] = jnp.zeros((pad_mesh - n_mesh, lat.shape[1]), BF)
        cot[n_mesh:] = jnp.zeros((pad_mesh - n_mesh, cot.shape[1]), BF)
    for f in fetches[0:12]:
        f.wait()
    table[:, 0:hidden] = dot(lat[...], w_mesh[...]).astype(BF)
    cot_terms = dot_t(cot[...], w_out[...])
    high = cot_terms.astype(BF)
    table[:, hidden : 2 * hidden] = high
    table[:, 2 * hidden :] = (cot_terms - high.astype(F32)).astype(BF)
    groups = 2 * half_edges // LANES
    per = block // LANES

    def step(i, carry):
        rows = pl.ds(pl.multiple_of(i * block, block), block)
        for c in range(per):
            at = index_row(i * per + c, groups, where)
            mine = slice(c * LANES, (c + 1) * LANES)
            edge_lanes = pl.ds(pl.multiple_of(i * block + c * LANES, LANES), LANES)
            slot = at * LANES + lax.broadcasted_iota(jnp.int32, (1, LANES), 1)
            row = local_receivers(receivers[pl.ds(at, 1), :], slot, where, piece)
            row = jnp.broadcast_to(row, (LANES, LANES))
            column = row.T
            for k in range(pad_mesh // LANES):
                left[mine, k * LANES : (k + 1) * LANES] = one_hot(column, k * LANES)
                at_row = n_grid + k * LANES
                right[at_row : at_row + LANES, edge_lanes] = one_hot_rows(row, k * LANES)
            row = local_senders(senders[pl.ds(at, 1), :], where, half_grid)
            row = jnp.broadcast_to(row, (LANES, LANES))
            for k in range(n_grid // LANES):
                right[k * LANES : (k + 1) * LANES, edge_lanes] = one_hot_rows(row, k * LANES)
        got = dot(left[...], table[...])
        pre = pre_part[rows, :] + got[:, 0:hidden]
        hidden_cot = got[:, hidden : 2 * hidden] + got[:, 2 * hidden :]
        sig = jax.nn.sigmoid(pre)
        act = (pre * sig).astype(BF)
        pre_cot = (hidden_cot * sig * (1.0 + pre * (1.0 - sig))).astype(BF)
        cots[rows, :] = pre_cot
        both[rows, 0:hidden] = pre_cot
        both[rows, hidden:] = act
        return carry

    lax.fori_loop(0, 2 * half_edges // block, step, 0)

    grid_tile = n_grid // 3
    mesh_tile = pad_mesh // 2

    def sum_grid(t, carry):
        at = pl.ds(pl.multiple_of(t * grid_tile, grid_tile), grid_tile)
        seg_grid[at, :] = dot(right[at, :], both[:, 0:hidden]).astype(BF)
        return carry

    def sum_mesh(t, carry):
        at = pl.multiple_of(t * mesh_tile, mesh_tile)
        sums[pl.ds(at, mesh_tile), :] = dot(right[pl.ds(n_grid + at, mesh_tile), :], both[...])
        return carry

    lax.fori_loop(0, 2, sum_mesh, 0)
    lax.fori_loop(0, 3, sum_grid, 0)
    for ref, o, kind in ((low_v, 0, BF), (rim_mid, 1, F32), (high_v, 2, BF)):
        for h in range(2):
            start = (3 * h + o) * piece
            ref[h * piece : (h + 1) * piece] = sums[start : start + piece, 0:hidden].astype(kind)
    rows = ROWS
    per_grad = w_mesh.shape[0] // rows
    parts = [slice(k * per_grad, (k + 1) * per_grad) for k in range(4)]
    stores = copies(
        [(low_v, rim_low), (high_v, rim_high)] + [(wire.at[p, 0 : 2 * ROWS + TAIL], wire_out.at[p]) for p in parts],
        out_sems,
    )
    for f in stores[0:2]:
        f.start()
    for f in fetches[12:] + copies(edges, edge_sems):
        f.wait()
    sub = lax.broadcasted_iota(jnp.int32, (16, LANES), 0)
    bias_total = dot(jnp.ones((16, 2 * half_edges), BF), both[:, 0:hidden])
    tail = jnp.where(sub == 0, bias_total[:, :LANES], jnp.where(sub == 1, bias_total[:, LANES:], 0.0)).astype(BF)
    for k in range(wire.shape[0]):
        wire[k, 2 * rows :, :] = tail

    def put_all(at, g):
        for k in range(g.shape[0] // rows):
            value = g[k * rows : (k + 1) * rows]
            wire[at + k, 0:rows, :] = value[:, :LANES].astype(BF)
            wire[at + k, rows : 2 * rows, :] = value[:, LANES:].astype(BF)

    put_all(parts[2].start, dot_rows(edge[...], both[:, 0:hidden]))
    stores[4].start()
    put_all(parts[0].start, dot_rows(grid[...], seg_grid[...]))
    stores[2].start()
    put_all(parts[1].start, dot_rows(lat[...], sums[:, 0:hidden].astype(BF)))
    stores[3].start()
    g = dot_rows(sums[:, hidden:].astype(BF), cot[...])
    put_all(parts[3].start, g[:, 0:hidden])
    put_all(parts[3].start + per_grad // 2, g[:, hidden:])
    stores[5].start()
    for f in stores:
        f.wait()


def swap(x):
    return lax.ppermute(x, "chan", [(0, 1), (1, 0)])


def pair_swap(x, first):
    n = lax.axis_size(BAND)
    pairs = [(i, i + 1) for i in range(first, n - 1, 2)]
    return lax.ppermute(x, BAND, pairs + [(j, i) for i, j in pairs])


def depth_total(mine):
    depth = lax.axis_size("zh")
    step = 1
    while True:
        mask = depth - 1 if 2 * step == depth else step
        other = lax.ppermute(mine, "zh", [(i, i ^ mask) for i in range(depth)])
        total = mine.astype(F32) + other.astype(F32)
        step *= 2
        if step == depth:
            return total
        mine = total.astype(BF)


def body(
    grid_latent,
    edge_latent,
    mesh_latent,
    mesh_cotangent,
    w_grid,
    w_mesh,
    w_edge,
    bias,
    w_out,
    senders,
    receivers,
    edge_count,
):
    band = lax.axis_index(BAND)
    chan = lax.axis_index("chan")
    half_grid = grid_latent.shape[0]
    half_edges = edge_latent.shape[0]
    piece, width = mesh_latent.shape
    hidden = w_grid.shape[1]
    n_grid = 2 * half_grid
    pad_mesh = -(-6 * piece // LANES) * LANES

    mesh_own = jnp.stack([mesh_latent, mesh_cotangent])
    mesh_low = pair_swap(mesh_own, 0)
    mesh_high = pair_swap(mesh_own, 1)
    edge_far = swap(edge_latent)
    grid_far = swap(grid_latent)
    mesh_own_far = swap(mesh_own)

    senders = senders.reshape(-1, LANES)
    receivers = receivers.reshape(-1, LANES)
    vmem = pl.BlockSpec(memory_space=pltpu.VMEM)
    smem = pl.BlockSpec(memory_space=pltpu.SMEM)
    small, large = [pltpu.CompilerParams(vmem_limit_bytes=n * 2**20) for n in (16, 40)]

    def near(x):
        return pltpu.with_memory_space_constraint(x, pltpu.VMEM)

    def wide(*arrays):
        return [pltpu.with_memory_space_constraint(x, pltpu.HBM) for x in arrays]

    def scalars(*arrays):
        return [pltpu.with_memory_space_constraint(x, pltpu.SMEM) for x in arrays]

    anywhere = pl.BlockSpec(memory_space=pl.ANY)
    dma = pltpu.SemaphoreType.DMA
    n_edges = 2 * half_edges
    pre = pl.pallas_call(
        sender_kernel,
        out_shape=pltpu.VMEM((n_edges, hidden), F32),
        in_specs=[smem] * 2 + [anywhere, vmem] * 2 + [anywhere] * 4,
        out_specs=vmem,
        scratch_shapes=[
            pltpu.VMEM((half_grid, width), BF),
            pltpu.VMEM((half_edges, width), BF),
            pltpu.VMEM((width, hidden), BF),
            pltpu.VMEM((1, hidden), F32),
            pltpu.VMEM(senders.shape, jnp.int32),
            pltpu.VMEM((n_grid + width, hidden), BF),
            pltpu.VMEM((EDGE_BLOCK, n_grid + width), BF),
            dma((6,)),
        ],
        compiler_params=small,
        cost_estimate=pl.CostEstimate(flops=SENDER_FLOPS, transcendentals=0, bytes_accessed=1 << 22),
        name="sender_step",
    )(
        *scalars(band.reshape(1), chan.reshape(1)),
        *wide(grid_latent),
        near(grid_far),
        *wide(edge_latent),
        near(edge_far),
        *wide(w_grid, w_edge, bias.reshape(1, hidden), senders),
    )

    mesh_low, mesh_high, pre = lax.optimization_barrier((mesh_low, mesh_high, pre))
    mesh_near = (mesh_low, mesh_own, mesh_high)
    mesh_far = [near(swap(mesh_low)), *wide(mesh_own_far), near(swap(mesh_high))]
    wire, cots, seg_grid, rim_low, rim_mid, rim_high = pl.pallas_call(
        edge_kernel,
        out_shape=(
            pltpu.HBM((MEMBERS, 2 * ROWS + TAIL, LANES), BF),
            pltpu.VMEM((n_edges, hidden), BF),
            pltpu.VMEM((n_grid, hidden), BF),
            pltpu.HBM((2 * piece, hidden), BF),
            pltpu.VMEM((2 * piece, hidden), F32),
            pltpu.HBM((2 * piece, hidden), BF),
        ),
        in_specs=[smem] * 3 + [anywhere] * 7 + [vmem, anywhere, vmem, anywhere, anywhere, vmem, anywhere, anywhere],
        out_specs=(anywhere, vmem, vmem, anywhere, vmem, anywhere),
        scratch_shapes=[
            pltpu.VMEM((n_grid, width), BF),
            pltpu.VMEM((n_edges, width), BF),
            pltpu.VMEM((pad_mesh, width), BF),
            pltpu.VMEM((pad_mesh, width), BF),
            pltpu.VMEM((pad_mesh, 3 * hidden), BF),
            pltpu.VMEM((EDGE_BLOCK, pad_mesh), BF),
            pltpu.VMEM((n_grid + pad_mesh, n_edges), BF),
            pltpu.VMEM((n_edges, 2 * hidden), BF),
            pltpu.VMEM((pad_mesh, 2 * hidden), F32),
            pltpu.VMEM((width, hidden), BF),
            pltpu.VMEM((hidden, width), BF),
            pltpu.VMEM(senders.shape, jnp.int32),
            pltpu.VMEM(receivers.shape, jnp.int32),
            pltpu.VMEM((MEMBERS, 2 * ROWS + 16, LANES), BF),
            pltpu.VMEM((2 * piece, hidden), BF),
            pltpu.VMEM((2 * piece, hidden), BF),
            dma((14,)),
            dma((n_edges // UNIT,)),
            dma((6,)),
        ],
        compiler_params=large,
        cost_estimate=pl.CostEstimate(flops=EDGE_FLOPS, transcendentals=1 << 20, bytes_accessed=1 << 23),
        name="edge_step",
    )(
        *scalars(band.reshape(1), chan.reshape(1), edge_count),
        *wide(grid_latent, grid_far, edge_latent, edge_far, *mesh_near),
        *mesh_far,
        *wide(w_mesh, w_out),
        near(pre),
        *wide(senders, receivers),
    )

    cot_own, cot_far = (cots[:half_edges], cots[half_edges:])
    from_low = pair_swap(rim_low, 0)
    from_high = pair_swap(rim_high, 1)
    arrived = lax.all_to_all(wire, GROUP, 0, 0, tiled=True)
    edge_term = dot_t(cot_far, w_edge).astype(BF)
    grid_term = dot_t(seg_grid[half_grid:], w_grid).astype(BF)
    edge_back = swap(edge_term)
    grid_back = swap(grid_term)
    total = arrived.astype(F32).sum(axis=0).astype(BF)
    total, from_low, from_high, _, _ = lax.optimization_barrier((total, from_low, from_high, edge_term, grid_term))
    total = depth_total(total)
    grad_bias = total[2 * ROWS : 2 * ROWS + 2].reshape(hidden)
    chunk = jnp.concatenate([total[:ROWS], total[ROWS : 2 * ROWS]], axis=1).astype(BF)
    spread = jnp.broadcast_to(chunk[None], (MEMBERS, ROWS, hidden))
    everyone = lax.all_to_all(spread, GROUP, 0, 0, tiled=True)

    grad_edge = (dot_t(cot_own, w_edge) + edge_back.astype(F32)).astype(BF)
    grad_grid = (dot_t(seg_grid[:half_grid], w_grid) + grid_back.astype(F32)).astype(BF)
    seg_mesh = (rim_mid + from_low.astype(F32) + from_high.astype(F32)).astype(BF)
    seg_mesh, _ = lax.optimization_barrier((seg_mesh, chunk))
    mesh_back = swap(dot_t(seg_mesh[piece:], w_mesh).astype(BF))
    grad_mesh = (dot_t(seg_mesh[:piece], w_mesh) + mesh_back.astype(F32)).astype(BF)

    def rows_of(start, stop):
        return everyone[start:stop].astype(F32).reshape(-1, hidden)

    q = MEMBERS // 4
    return (
        grad_grid,
        grad_edge,
        grad_mesh,
        rows_of(0, q),
        rows_of(q, 2 * q),
        rows_of(2 * q, 3 * q),
        grad_bias,
        jnp.concatenate([rows_of(3 * q, 3 * q + q // 2), rows_of(3 * q + q // 2, 4 * q)], axis=1),
    )


def solution(mesh):
    bands, chans = (mesh.shape["band"], mesh.shape["chan"])
    side = 4
    inner = Mesh(np.asarray(mesh.devices).reshape(bands // (2 * side**2), 2, side, side, chans), (*BAND, "chan"))
    every = P((*BAND, "chan"), None)
    return jax.shard_map(
        body,
        mesh=inner,
        in_specs=(
            every,
            every,
            every,
            every,
            P(None, "chan"),
            P(None, "chan"),
            P(None, "chan"),
            P("chan"),
            P("chan", None),
            P(BAND),
            P(BAND),
            P(BAND),
        ),
        out_specs=(
            every,
            every,
            every,
            P(None, "chan"),
            P(None, "chan"),
            P(None, "chan"),
            P("chan"),
            P("chan", None),
        ),
        check_vma=False,
    )
```

```python
import functools

import jax
import jax.numpy as jnp
import numpy as np
from jax import lax
from jax.experimental import pallas as pl
from jax.experimental.pallas import tpu as pltpu
from jax.sharding import Mesh, PartitionSpec as P

BF = jnp.bfloat16
F32 = jnp.float32
BAND = ("zh", "zl", "y", "x")
GROUP = ("zl", "y", "x")
LANES = 128
EDGE_BLOCK = 768
UNIT = 384
TAIL = 8
ROWS = 64
MEMBERS = 32
SENDER_FLOPS = 4 * 10**9
EDGE_FLOPS = 9 * 10**9


def dot(a, b):
    return jnp.dot(a, b, preferred_element_type=F32)


def dot_t(a, b):
    return lax.dot_general(a, b, (((1,), (1,)), ((), ())), preferred_element_type=F32)


def dot_rows(a, b):
    return lax.dot_general(a, b, (((0,), (0,)), ((), ())), preferred_element_type=F32)


def one_hot(column, offset):
    place = lax.broadcasted_iota(jnp.int32, column.shape, column.ndim - 1)
    return jnp.where(column == place + offset, 1.0, 0.0).astype(BF)


def one_hot_rows(row, offset):
    place = lax.broadcasted_iota(jnp.int32, row.shape, 0)
    return jnp.where(row == place + offset, 1.0, 0.0).astype(BF)


def local_senders(row, where, half_grid):
    at = row - where[0] * (2 * half_grid) - where[1] * half_grid
    return jnp.where(at < 0, at + 2 * half_grid, at)


def local_receivers(row, slot, where, piece):
    at = row - (where[0] - 1) * (2 * piece)
    owner = jnp.where(at >= 2 * piece, 1, 0) + jnp.where(at >= 4 * piece, 1, 0)
    within = at - owner * (2 * piece)
    half = jnp.where(within >= piece, 1, 0)
    flip = jnp.where(half == where[1], 0, 1)
    place = jnp.where(where[0] % 2 == 0, 2 - owner, owner)
    near = (flip * 3 + place) * piece + within - half * piece
    return jnp.where(slot < where[2], near, -1)


def index_row(group, groups, where):
    at = group + where[1] * (groups // 2)
    return jnp.where(at >= groups, at - groups, at)


def copies(pairs, sems):
    return [pltpu.make_async_copy(src, dst, sems.at[k]) for k, (src, dst) in enumerate(pairs)]


def sender_kernel(
    piece,
    band,
    chan,
    count,
    grid_own,
    grid_far,
    edge_own,
    edge_far,
    w_grid,
    w_edge,
    bias_in,
    send_in,
    recv_in,
    pre,
    left_mesh,
    right,
    grid,
    edge,
    weights,
    bias_row,
    senders,
    receivers,
    table,
    left,
    in_sems,
):
    where = (band[0], chan[0], count[0])
    half_edges = edge_own.shape[0]
    half_grid = grid_own.shape[0]
    n_grid = 2 * half_grid
    block = left.shape[0]
    fetches = copies(
        (
            (w_grid, weights),
            (grid_own, grid),
            (send_in, senders),
            (recv_in, receivers),
            (w_edge, table.at[n_grid:]),
            (bias_in, bias_row),
            (edge_own, edge),
        ),
        in_sems,
    )
    for f in fetches:
        f.start()
    fetches[0].wait()
    table[half_grid:n_grid] = dot(grid_far[...], weights[...]).astype(BF)
    fetches[1].wait()
    table[0:half_grid] = dot(grid[...], weights[...]).astype(BF)
    for f in fetches[2:]:
        f.wait()
    groups = 2 * half_edges // LANES
    per = block // LANES
    units = block // UNIT
    near = half_edges // UNIT

    def step(i, carry):
        rows = pl.ds(pl.multiple_of(i * block, block), block)
        for h in range(units):
            at = i * units + h
            mine = slice(h * UNIT, (h + 1) * UNIT)

            @pl.when(at < near)
            def _():
                left[mine, n_grid:] = edge[pl.ds(pl.multiple_of(at * UNIT, UNIT), UNIT), :]

            @pl.when(at >= near)
            def _():
                left[mine, n_grid:] = edge_far[pl.ds(pl.multiple_of((at - near) * UNIT, UNIT), UNIT), :]

        for c in range(per):
            at = index_row(i * per + c, groups, where)
            mine = pl.ds(pl.multiple_of(i * block + c * LANES, LANES), LANES)
            row = local_senders(senders[pl.ds(at, 1), :], where, half_grid)
            row = jnp.broadcast_to(row, (LANES, LANES))
            column = row.T
            for k in range(n_grid // LANES):
                left[c * LANES : (c + 1) * LANES, k * LANES : (k + 1) * LANES] = one_hot(column, k * LANES)
                right[k * LANES : (k + 1) * LANES, mine] = one_hot_rows(row, k * LANES)
            slot = at * LANES + lax.broadcasted_iota(jnp.int32, (1, LANES), 1)
            row = local_receivers(receivers[pl.ds(at, 1), :], slot, where, piece)
            row = jnp.broadcast_to(row, (LANES, LANES))
            column = row.T
            for k in range(left_mesh.shape[1] // LANES):
                left_mesh[mine, k * LANES : (k + 1) * LANES] = one_hot(column, k * LANES)
                at_row = n_grid + k * LANES
                right[at_row : at_row + LANES, mine] = one_hot_rows(row, k * LANES)
        pre[rows, :] = dot(left[...], table[...]) + bias_row[...]
        return carry

    lax.fori_loop(0, 2 * half_edges // block, step, 0)


def edge_kernel(
    grid_own,
    grid_far,
    edge_own,
    edge_far,
    m0,
    m1,
    m2,
    m3,
    m4,
    m5,
    w_mesh_in,
    w_out_in,
    pre_part,
    left,
    right,
    wire_out,
    cots,
    seg_grid,
    rim_low,
    rim_mid,
    rim_high,
    grid,
    edge,
    lat,
    cot,
    table,
    both,
    sums,
    w_mesh,
    w_out,
    wire,
    low_v,
    high_v,
    in_sems,
    edge_sems,
    out_sems,
):
    half_edges = edge_own.shape[0]
    half_grid = grid_own.shape[0]
    n_grid = 2 * half_grid
    piece = m0.shape[1]
    n_mesh = 6 * piece
    pad_mesh = lat.shape[0]
    n_rows = n_grid + pad_mesh
    block = EDGE_BLOCK
    hidden = w_mesh.shape[1]
    near = half_edges // UNIT
    apart = ((0, m0), (1, m1), (2, m2), (4, m4))
    lats = [(m.at[0], lat.at[k * piece : (k + 1) * piece]) for k, m in apart]
    cot_pairs = [(m.at[1], cot.at[k * piece : (k + 1) * piece]) for k, m in apart]
    grids = [(grid_own, grid.at[0:half_grid]), (grid_far, grid.at[half_grid:])]
    small = [(w_mesh_in, w_mesh), (w_out_in, w_out)]
    fetches = copies(small + lats + cot_pairs + grids, in_sems)
    edges = [
        (source.at[k * UNIT : (k + 1) * UNIT], edge.at[(k + off) * UNIT : (k + off + 1) * UNIT])
        for source, off in ((edge_own, 0), (edge_far, near))
        for k in range(near)
    ]
    for f in fetches[0:10] + copies(edges, edge_sems) + fetches[10:]:
        f.start()
    for k, m in ((3, m3), (5, m5)):
        lat[k * piece : (k + 1) * piece] = m[0]
        cot[k * piece : (k + 1) * piece] = m[1]
    if pad_mesh > n_mesh:
        lat[n_mesh:] = jnp.zeros((pad_mesh - n_mesh, lat.shape[1]), BF)
        cot[n_mesh:] = jnp.zeros((pad_mesh - n_mesh, cot.shape[1]), BF)
    for f in fetches[0:10]:
        f.wait()
    table[:, 0:hidden] = dot(lat[...], w_mesh[...]).astype(BF)
    cot_terms = dot_t(cot[...], w_out[...])
    high = cot_terms.astype(BF)
    table[:, hidden : 2 * hidden] = high
    table[:, 2 * hidden :] = (cot_terms - high.astype(F32)).astype(BF)
    def step(i, carry):
        rows = pl.ds(pl.multiple_of(i * block, block), block)
        got = dot(left[rows, :], table[...])
        pre = pre_part[rows, :] + got[:, 0:hidden]
        hidden_cot = got[:, hidden : 2 * hidden] + got[:, 2 * hidden :]
        sig = jax.nn.sigmoid(pre)
        act = (pre * sig).astype(BF)
        pre_cot = (hidden_cot * sig * (1.0 + pre * (1.0 - sig))).astype(BF)
        cots[rows, :] = pre_cot
        both[rows, 0:hidden] = pre_cot
        both[rows, hidden:] = act
        return carry

    lax.fori_loop(0, 2 * half_edges // block, step, 0)

    grid_tile = n_grid // 3
    mesh_tile = pad_mesh // 2

    def sum_grid(t, carry):
        at = pl.ds(pl.multiple_of(t * grid_tile, grid_tile), grid_tile)
        seg_grid[at, :] = dot(right[at, :], both[:, 0:hidden]).astype(BF)
        return carry

    def sum_mesh(t, carry):
        at = pl.multiple_of(t * mesh_tile, mesh_tile)
        sums[pl.ds(at, mesh_tile), :] = dot(right[pl.ds(n_grid + at, mesh_tile), :], both[...])
        return carry

    lax.fori_loop(0, 2, sum_mesh, 0)
    lax.fori_loop(0, 3, sum_grid, 0)
    for ref, o, kind in ((low_v, 0, BF), (rim_mid, 1, F32), (high_v, 2, BF)):
        for h in range(2):
            start = (3 * h + o) * piece
            ref[h * piece : (h + 1) * piece] = sums[start : start + piece, 0:hidden].astype(kind)
    rows = ROWS
    per_grad = w_mesh.shape[0] // rows
    parts = [slice(k * per_grad, (k + 1) * per_grad) for k in range(4)]
    stores = copies(
        [(low_v, rim_low), (high_v, rim_high)] + [(wire.at[p, 0 : 2 * ROWS + TAIL], wire_out.at[p]) for p in parts],
        out_sems,
    )
    for f in stores[0:2]:
        f.start()
    for f in fetches[10:] + copies(edges, edge_sems):
        f.wait()
    sub = lax.broadcasted_iota(jnp.int32, (16, LANES), 0)
    bias_total = dot(jnp.ones((16, 2 * half_edges), BF), both[:, 0:hidden])
    tail = jnp.where(sub == 0, bias_total[:, :LANES], jnp.where(sub == 1, bias_total[:, LANES:], 0.0)).astype(BF)
    for k in range(wire.shape[0]):
        wire[k, 2 * rows :, :] = tail

    def put_all(at, g):
        for k in range(g.shape[0] // rows):
            value = g[k * rows : (k + 1) * rows]
            wire[at + k, 0:rows, :] = value[:, :LANES].astype(BF)
            wire[at + k, rows : 2 * rows, :] = value[:, LANES:].astype(BF)

    put_all(parts[2].start, dot_rows(edge[...], both[:, 0:hidden]))
    stores[4].start()
    put_all(parts[0].start, dot_rows(grid[...], seg_grid[...]))
    stores[2].start()
    put_all(parts[1].start, dot_rows(lat[...], sums[:, 0:hidden].astype(BF)))
    stores[3].start()
    g = dot_rows(sums[:, hidden:].astype(BF), cot[...])
    put_all(parts[3].start, g[:, 0:hidden])
    put_all(parts[3].start + per_grad // 2, g[:, hidden:])
    stores[5].start()
    for f in stores:
        f.wait()


def swap(x):
    return lax.ppermute(x, "chan", [(0, 1), (1, 0)])


def pair_swap(x, first):
    n = lax.axis_size(BAND)
    pairs = [(i, i + 1) for i in range(first, n - 1, 2)]
    return lax.ppermute(x, BAND, pairs + [(j, i) for i, j in pairs])


def depth_total(mine):
    depth = lax.axis_size("zh")
    step = 1
    while True:
        mask = depth - 1 if 2 * step == depth else step
        other = lax.ppermute(mine, "zh", [(i, i ^ mask) for i in range(depth)])
        total = mine.astype(F32) + other.astype(F32)
        step *= 2
        if step == depth:
            return total
        mine = total.astype(BF)


def body(
    grid_latent,
    edge_latent,
    mesh_latent,
    mesh_cotangent,
    w_grid,
    w_mesh,
    w_edge,
    bias,
    w_out,
    senders,
    receivers,
    edge_count,
):
    band = lax.axis_index(BAND)
    chan = lax.axis_index("chan")
    half_grid = grid_latent.shape[0]
    half_edges = edge_latent.shape[0]
    piece, width = mesh_latent.shape
    hidden = w_grid.shape[1]
    n_grid = 2 * half_grid
    pad_mesh = -(-6 * piece // LANES) * LANES

    mesh_own = jnp.stack([mesh_latent, mesh_cotangent])
    mesh_low = pair_swap(mesh_own, 0)
    mesh_high = pair_swap(mesh_own, 1)
    edge_far = swap(edge_latent)
    grid_far = swap(grid_latent)
    mesh_own_far = swap(mesh_own)

    senders = senders.reshape(-1, LANES)
    receivers = receivers.reshape(-1, LANES)
    vmem = pl.BlockSpec(memory_space=pltpu.VMEM)
    smem = pl.BlockSpec(memory_space=pltpu.SMEM)
    small, large = [pltpu.CompilerParams(vmem_limit_bytes=n * 2**20) for n in (12, 26)]

    def near(x):
        return pltpu.with_memory_space_constraint(x, pltpu.VMEM)

    def wide(*arrays):
        return [pltpu.with_memory_space_constraint(x, pltpu.HBM) for x in arrays]

    def scalars(*arrays):
        return [pltpu.with_memory_space_constraint(x, pltpu.SMEM) for x in arrays]

    anywhere = pl.BlockSpec(memory_space=pl.ANY)
    dma = pltpu.SemaphoreType.DMA
    n_edges = 2 * half_edges
    pre, left, right = pl.pallas_call(
        functools.partial(sender_kernel, piece),
        out_shape=(
            pltpu.VMEM((n_edges, hidden), F32),
            pltpu.VMEM((n_edges, pad_mesh), BF),
            pltpu.VMEM((n_grid + pad_mesh, n_edges), BF),
        ),
        in_specs=[smem] * 3 + [anywhere, vmem] * 2 + [anywhere] * 5,
        out_specs=(vmem,) * 3,
        scratch_shapes=[
            pltpu.VMEM((half_grid, width), BF),
            pltpu.VMEM((half_edges, width), BF),
            pltpu.VMEM((width, hidden), BF),
            pltpu.VMEM((1, hidden), F32),
            pltpu.VMEM(senders.shape, jnp.int32),
            pltpu.VMEM(receivers.shape, jnp.int32),
            pltpu.VMEM((n_grid + width, hidden), BF),
            pltpu.VMEM((EDGE_BLOCK, n_grid + width), BF),
            dma((7,)),
        ],
        compiler_params=small,
        cost_estimate=pl.CostEstimate(flops=SENDER_FLOPS, transcendentals=0, bytes_accessed=1 << 22),
        name="sender_step",
    )(
        *scalars(band.reshape(1), chan.reshape(1), edge_count),
        *wide(grid_latent),
        near(grid_far),
        *wide(edge_latent),
        near(edge_far),
        *wide(w_grid, w_edge, bias.reshape(1, hidden), senders, receivers),
    )

    mesh_low, mesh_high, pre, left, right = lax.optimization_barrier((mesh_low, mesh_high, pre, left, right))
    mesh_near = (mesh_low, mesh_own, mesh_high)
    mesh_far = [near(swap(mesh_low)), *wide(mesh_own_far), near(swap(mesh_high))]
    wire, cots, seg_grid, rim_low, rim_mid, rim_high = pl.pallas_call(
        edge_kernel,
        out_shape=(
            pltpu.HBM((MEMBERS, 2 * ROWS + TAIL, LANES), BF),
            pltpu.VMEM((n_edges, hidden), BF),
            pltpu.VMEM((n_grid, hidden), BF),
            pltpu.HBM((2 * piece, hidden), BF),
            pltpu.VMEM((2 * piece, hidden), F32),
            pltpu.HBM((2 * piece, hidden), BF),
        ),
        in_specs=[anywhere] * 7 + [vmem, anywhere, vmem, anywhere, anywhere, vmem, vmem, vmem],
        out_specs=(anywhere, vmem, vmem, anywhere, vmem, anywhere),
        scratch_shapes=[
            pltpu.VMEM((n_grid, width), BF),
            pltpu.VMEM((n_edges, width), BF),
            pltpu.VMEM((pad_mesh, width), BF),
            pltpu.VMEM((pad_mesh, width), BF),
            pltpu.VMEM((pad_mesh, 3 * hidden), BF),
            pltpu.VMEM((n_edges, 2 * hidden), BF),
            pltpu.VMEM((pad_mesh, 2 * hidden), F32),
            pltpu.VMEM((width, hidden), BF),
            pltpu.VMEM((hidden, width), BF),
            pltpu.VMEM((MEMBERS, 2 * ROWS + 16, LANES), BF),
            pltpu.VMEM((2 * piece, hidden), BF),
            pltpu.VMEM((2 * piece, hidden), BF),
            dma((12,)),
            dma((n_edges // UNIT,)),
            dma((6,)),
        ],
        compiler_params=large,
        cost_estimate=pl.CostEstimate(flops=EDGE_FLOPS, transcendentals=1 << 20, bytes_accessed=1 << 23),
        name="edge_step",
    )(
        *wide(grid_latent, grid_far, edge_latent, edge_far, *mesh_near),
        *mesh_far,
        *wide(w_mesh, w_out),
        near(pre),
        near(left),
        near(right),
    )

    cot_own, cot_far = (cots[:half_edges], cots[half_edges:])
    from_low = pair_swap(rim_low, 0)
    from_high = pair_swap(rim_high, 1)
    arrived = lax.all_to_all(wire, GROUP, 0, 0, tiled=True)
    edge_term = dot_t(cot_far, w_edge).astype(BF)
    grid_term = dot_t(seg_grid[half_grid:], w_grid).astype(BF)
    edge_back = swap(edge_term)
    grid_back = swap(grid_term)
    total = arrived.astype(F32).sum(axis=0).astype(BF)
    total, from_low, from_high, _, _ = lax.optimization_barrier((total, from_low, from_high, edge_term, grid_term))
    total = depth_total(total)
    grad_bias = total[2 * ROWS : 2 * ROWS + 2].reshape(hidden)
    chunk = jnp.concatenate([total[:ROWS], total[ROWS : 2 * ROWS]], axis=1).astype(BF)
    spread = jnp.broadcast_to(chunk[None], (MEMBERS, ROWS, hidden))
    everyone = lax.all_to_all(spread, GROUP, 0, 0, tiled=True)

    grad_edge = (dot_t(cot_own, w_edge) + edge_back.astype(F32)).astype(BF)
    grad_grid = (dot_t(seg_grid[:half_grid], w_grid) + grid_back.astype(F32)).astype(BF)
    seg_mesh = (rim_mid + from_low.astype(F32) + from_high.astype(F32)).astype(BF)
    seg_mesh, _ = lax.optimization_barrier((seg_mesh, chunk))
    mesh_back = swap(dot_t(seg_mesh[piece:], w_mesh).astype(BF))
    grad_mesh = (dot_t(seg_mesh[:piece], w_mesh) + mesh_back.astype(F32)).astype(BF)

    def rows_of(start, stop):
        return everyone[start:stop].astype(F32).reshape(-1, hidden)

    q = MEMBERS // 4
    return (
        grad_grid,
        grad_edge,
        grad_mesh,
        rows_of(0, q),
        rows_of(q, 2 * q),
        rows_of(2 * q, 3 * q),
        grad_bias,
        jnp.concatenate([rows_of(3 * q, 3 * q + q // 2), rows_of(3 * q + q // 2, 4 * q)], axis=1),
    )


def solution(mesh):
    bands, chans = (mesh.shape["band"], mesh.shape["chan"])
    side = 4
    inner = Mesh(np.asarray(mesh.devices).reshape(bands // (2 * side**2), 2, side, side, chans), (*BAND, "chan"))
    every = P((*BAND, "chan"), None)
    return jax.shard_map(
        body,
        mesh=inner,
        in_specs=(
            every,
            every,
            every,
            every,
            P(None, "chan"),
            P(None, "chan"),
            P(None, "chan"),
            P("chan"),
            P("chan", None),
            P(BAND),
            P(BAND),
            P(BAND),
        ),
        out_specs=(
            every,
            every,
            every,
            P(None, "chan"),
            P(None, "chan"),
            P(None, "chan"),
            P("chan"),
            P("chan", None),
        ),
        check_vma=False,
    )
```

```python
import functools

import jax
import jax.numpy as jnp
import numpy as np
from jax import lax
from jax.experimental import pallas as pl
from jax.experimental.pallas import tpu as pltpu
from jax.sharding import Mesh, PartitionSpec as P

BF = jnp.bfloat16
F32 = jnp.float32
BAND = ("zh", "zl", "y", "x")
GROUP = ("zl", "y", "x")
LANES = 128
EDGE_BLOCK = 768
UNIT = 384
TAIL = 8
ROWS = 64
MEMBERS = 32
SENDER_FLOPS = 4 * 10**9
EDGE_FLOPS = 9 * 10**9


def dot(a, b):
    return jnp.dot(a, b, preferred_element_type=F32)


def dot_t(a, b):
    return lax.dot_general(a, b, (((1,), (1,)), ((), ())), preferred_element_type=F32)


def dot_rows(a, b):
    return lax.dot_general(a, b, (((0,), (0,)), ((), ())), preferred_element_type=F32)


def one_hot(column, offset):
    place = lax.broadcasted_iota(jnp.int32, column.shape, column.ndim - 1)
    return jnp.where(column == place + offset, 1.0, 0.0).astype(BF)


def one_hot_rows(row, offset):
    place = lax.broadcasted_iota(jnp.int32, row.shape, 0)
    return jnp.where(row == place + offset, 1.0, 0.0).astype(BF)


def local_senders(row, where, half_grid):
    at = row - where[0] * (2 * half_grid) - where[1] * half_grid
    return jnp.where(at < 0, at + 2 * half_grid, at)


def local_receivers(row, slot, where, piece):
    at = row - (where[0] - 1) * (2 * piece)
    owner = jnp.where(at >= 2 * piece, 1, 0) + jnp.where(at >= 4 * piece, 1, 0)
    within = at - owner * (2 * piece)
    half = jnp.where(within >= piece, 1, 0)
    flip = jnp.where(half == where[1], 0, 1)
    place = jnp.where(where[0] % 2 == 0, 2 - owner, owner)
    near = (flip * 3 + place) * piece + within - half * piece
    return jnp.where(slot < where[2], near, -1)


def index_row(group, groups, where):
    at = group + where[1] * (groups // 2)
    return jnp.where(at >= groups, at - groups, at)


def copies(pairs, sems):
    return [pltpu.make_async_copy(src, dst, sems.at[k]) for k, (src, dst) in enumerate(pairs)]


def sender_kernel(
    piece,
    band,
    chan,
    count,
    grid_own,
    grid_far,
    edge_own,
    edge_far,
    w_grid,
    w_edge,
    bias_in,
    send_in,
    recv_in,
    pre,
    left_mesh,
    right,
    grid,
    edge,
    weights,
    bias_row,
    senders,
    receivers,
    table,
    left,
    in_sems,
):
    where = (band[0], chan[0], count[0])
    half_edges = edge_own.shape[0]
    half_grid = grid_own.shape[0]
    n_grid = 2 * half_grid
    block = left.shape[0]
    fetches = copies(
        (
            (w_grid, weights),
            (grid_own, grid),
            (send_in, senders),
            (recv_in, receivers),
            (w_edge, table.at[n_grid:]),
            (bias_in, bias_row),
            (edge_own, edge),
        ),
        in_sems,
    )
    for f in fetches:
        f.start()
    fetches[0].wait()
    table[half_grid:n_grid] = dot(grid_far[...], weights[...]).astype(BF)
    fetches[1].wait()
    table[0:half_grid] = dot(grid[...], weights[...]).astype(BF)
    for f in fetches[2:]:
        f.wait()
    groups = 2 * half_edges // LANES
    per = block // LANES
    units = block // UNIT
    near = half_edges // UNIT

    def step(i, carry):
        rows = pl.ds(pl.multiple_of(i * block, block), block)
        for h in range(units):
            at = i * units + h
            mine = slice(h * UNIT, (h + 1) * UNIT)

            @pl.when(at < near)
            def _():
                left[mine, n_grid:] = edge[pl.ds(pl.multiple_of(at * UNIT, UNIT), UNIT), :]

            @pl.when(at >= near)
            def _():
                left[mine, n_grid:] = edge_far[pl.ds(pl.multiple_of((at - near) * UNIT, UNIT), UNIT), :]

        for c in range(per):
            at = index_row(i * per + c, groups, where)
            mine = pl.ds(pl.multiple_of(i * block + c * LANES, LANES), LANES)
            row = local_senders(senders[pl.ds(at, 1), :], where, half_grid)
            row = jnp.broadcast_to(row, (LANES, LANES))
            column = row.T
            for k in range(n_grid // LANES):
                left[c * LANES : (c + 1) * LANES, k * LANES : (k + 1) * LANES] = one_hot(column, k * LANES)
                right[k * LANES : (k + 1) * LANES, mine] = one_hot_rows(row, k * LANES)
            slot = at * LANES + lax.broadcasted_iota(jnp.int32, (1, LANES), 1)
            row = local_receivers(receivers[pl.ds(at, 1), :], slot, where, piece)
            row = jnp.broadcast_to(row, (LANES, LANES))
            column = row.T
            for k in range(left_mesh.shape[1] // LANES):
                left_mesh[mine, k * LANES : (k + 1) * LANES] = one_hot(column, k * LANES)
                at_row = n_grid + k * LANES
                right[at_row : at_row + LANES, mine] = one_hot_rows(row, k * LANES)
        pre[rows, :] = dot(left[...], table[...]) + bias_row[...]
        return carry

    lax.fori_loop(0, 2 * half_edges // block, step, 0)


def edge_kernel(
    grid_own,
    grid_far,
    edge_own,
    edge_far,
    m0,
    m1,
    m2,
    m3,
    m4,
    m5,
    w_mesh_in,
    w_out_in,
    pre_part,
    left,
    right,
    wire_out,
    cots,
    seg_grid,
    rim_low,
    rim_mid,
    rim_high,
    grid,
    edge,
    lat,
    cot,
    table,
    both,
    sums,
    w_mesh,
    w_out,
    wire,
    low_v,
    high_v,
    in_sems,
    edge_sems,
    out_sems,
):
    half_edges = edge_own.shape[0]
    half_grid = grid_own.shape[0]
    n_grid = 2 * half_grid
    piece = m0.shape[1]
    n_mesh = 6 * piece
    pad_mesh = lat.shape[0]
    n_rows = n_grid + pad_mesh
    block = EDGE_BLOCK
    hidden = w_mesh.shape[1]
    near = half_edges // UNIT
    apart = ((0, m0), (1, m1), (2, m2), (4, m4))
    lats = [(m.at[0], lat.at[k * piece : (k + 1) * piece]) for k, m in apart]
    cot_pairs = [(m.at[1], cot.at[k * piece : (k + 1) * piece]) for k, m in apart]
    grids = [(grid_own, grid.at[0:half_grid]), (grid_far, grid.at[half_grid:])]
    small = [(w_mesh_in, w_mesh), (w_out_in, w_out)]
    fetches = copies(small + lats + cot_pairs + grids, in_sems)
    edges = [
        (source.at[k * UNIT : (k + 1) * UNIT], edge.at[(k + off) * UNIT : (k + off + 1) * UNIT])
        for source, off in ((edge_own, 0), (edge_far, near))
        for k in range(near)
    ]
    for f in fetches[0:10] + copies(edges, edge_sems) + fetches[10:]:
        f.start()
    for k, m in ((3, m3), (5, m5)):
        lat[k * piece : (k + 1) * piece] = m[0]
        cot[k * piece : (k + 1) * piece] = m[1]
    if pad_mesh > n_mesh:
        lat[n_mesh:] = jnp.zeros((pad_mesh - n_mesh, lat.shape[1]), BF)
        cot[n_mesh:] = jnp.zeros((pad_mesh - n_mesh, cot.shape[1]), BF)
    for f in fetches[0:10]:
        f.wait()
    table[:, 0:hidden] = dot(lat[...], w_mesh[...]).astype(BF)
    cot_terms = dot_t(cot[...], w_out[...])
    high = cot_terms.astype(BF)
    table[:, hidden : 2 * hidden] = high
    table[:, 2 * hidden :] = (cot_terms - high.astype(F32)).astype(BF)
    def step(i, carry):
        rows = pl.ds(pl.multiple_of(i * block, block), block)
        got = dot(left[rows, :], table[...])
        pre = pre_part[rows, :] + got[:, 0:hidden]
        hidden_cot = got[:, hidden : 2 * hidden] + got[:, 2 * hidden :]
        sig = jax.nn.sigmoid(pre)
        act = (pre * sig).astype(BF)
        pre_cot = (hidden_cot * sig * (1.0 + pre * (1.0 - sig))).astype(BF)
        cots[rows, :] = pre_cot
        both[rows, 0:hidden] = pre_cot
        both[rows, hidden:] = act
        return carry

    lax.fori_loop(0, 2 * half_edges // block, step, 0)

    grid_tile = n_grid // 3
    mesh_tile = pad_mesh // 2

    def sum_grid(t, carry):
        at = pl.ds(pl.multiple_of(t * grid_tile, grid_tile), grid_tile)
        seg_grid[at, :] = dot(right[at, :], both[:, 0:hidden]).astype(BF)
        return carry

    def sum_mesh(t, carry):
        at = pl.multiple_of(t * mesh_tile, mesh_tile)
        sums[pl.ds(at, mesh_tile), :] = dot(right[pl.ds(n_grid + at, mesh_tile), :], both[...])
        return carry

    lax.fori_loop(0, 2, sum_mesh, 0)
    lax.fori_loop(0, 3, sum_grid, 0)
    for ref, o, kind in ((low_v, 0, BF), (rim_mid, 1, F32), (high_v, 2, BF)):
        for h in range(2):
            start = (3 * h + o) * piece
            ref[h * piece : (h + 1) * piece] = sums[start : start + piece, 0:hidden].astype(kind)
    rows = ROWS
    per_grad = w_mesh.shape[0] // rows
    parts = [slice(k * per_grad, (k + 1) * per_grad) for k in range(4)]
    stores = copies(
        [(low_v, rim_low), (high_v, rim_high)] + [(wire.at[p, 0 : 2 * ROWS + TAIL], wire_out.at[p]) for p in parts],
        out_sems,
    )
    for f in stores[0:2]:
        f.start()
    for f in fetches[10:] + copies(edges, edge_sems):
        f.wait()
    sub = lax.broadcasted_iota(jnp.int32, (16, LANES), 0)
    bias_total = dot(jnp.ones((16, 2 * half_edges), BF), both[:, 0:hidden])
    tail = jnp.where(sub == 0, bias_total[:, :LANES], jnp.where(sub == 1, bias_total[:, LANES:], 0.0)).astype(BF)
    for k in range(wire.shape[0]):
        wire[k, 2 * rows :, :] = tail

    def put_all(at, g):
        for k in range(g.shape[0] // rows):
            value = g[k * rows : (k + 1) * rows]
            wire[at + k, 0:rows, :] = value[:, :LANES].astype(BF)
            wire[at + k, rows : 2 * rows, :] = value[:, LANES:].astype(BF)

    put_all(parts[2].start, dot_rows(edge[...], both[:, 0:hidden]))
    stores[4].start()
    put_all(parts[0].start, dot_rows(grid[...], seg_grid[...]))
    stores[2].start()
    put_all(parts[1].start, dot_rows(lat[...], sums[:, 0:hidden].astype(BF)))
    stores[3].start()
    g = dot_rows(sums[:, hidden:].astype(BF), cot[...])
    put_all(parts[3].start, g[:, 0:hidden])
    put_all(parts[3].start + per_grad // 2, g[:, hidden:])
    stores[5].start()
    for f in stores:
        f.wait()


def swap(x):
    return lax.ppermute(x, "chan", [(0, 1), (1, 0)])


def pair_swap(x, first):
    n = lax.axis_size(BAND)
    pairs = [(i, i + 1) for i in range(first, n - 1, 2)]
    return lax.ppermute(x, BAND, pairs + [(j, i) for i, j in pairs])


def depth_total(mine):
    depth = lax.axis_size("zh")
    step = 1
    while True:
        mask = depth - 1 if 2 * step == depth else step
        other = lax.ppermute(mine, "zh", [(i, i ^ mask) for i in range(depth)])
        total = mine.astype(F32) + other.astype(F32)
        step *= 2
        if step == depth:
            return total
        mine = total.astype(BF)


def body(
    grid_latent,
    edge_latent,
    mesh_latent,
    mesh_cotangent,
    w_grid,
    w_mesh,
    w_edge,
    bias,
    w_out,
    senders,
    receivers,
    edge_count,
):
    band = lax.axis_index(BAND)
    chan = lax.axis_index("chan")
    half_grid = grid_latent.shape[0]
    half_edges = edge_latent.shape[0]
    piece, width = mesh_latent.shape
    hidden = w_grid.shape[1]
    n_grid = 2 * half_grid
    pad_mesh = -(-6 * piece // LANES) * LANES

    mesh_own = jnp.stack([mesh_latent, mesh_cotangent])
    mesh_low = pair_swap(mesh_own, 0)
    mesh_high = pair_swap(mesh_own, 1)
    edge_far = swap(edge_latent)
    grid_far = swap(grid_latent)
    mesh_own_far = swap(mesh_own)

    senders = senders.reshape(-1, LANES)
    receivers = receivers.reshape(-1, LANES)
    vmem = pl.BlockSpec(memory_space=pltpu.VMEM)
    smem = pl.BlockSpec(memory_space=pltpu.SMEM)
    small, large = [pltpu.CompilerParams(vmem_limit_bytes=n * 2**20) for n in (12, 26)]

    def near(x):
        return pltpu.with_memory_space_constraint(x, pltpu.VMEM)

    def wide(*arrays):
        return [pltpu.with_memory_space_constraint(x, pltpu.HBM) for x in arrays]

    def scalars(*arrays):
        return [pltpu.with_memory_space_constraint(x, pltpu.SMEM) for x in arrays]

    anywhere = pl.BlockSpec(memory_space=pl.ANY)
    dma = pltpu.SemaphoreType.DMA
    n_edges = 2 * half_edges
    pre, left, right = pl.pallas_call(
        functools.partial(sender_kernel, piece),
        out_shape=(
            pltpu.VMEM((n_edges, hidden), F32),
            pltpu.VMEM((n_edges, pad_mesh), BF),
            pltpu.VMEM((n_grid + pad_mesh, n_edges), BF),
        ),
        in_specs=[smem] * 3 + [anywhere, vmem] * 2 + [anywhere] * 5,
        out_specs=(vmem,) * 3,
        scratch_shapes=[
            pltpu.VMEM((half_grid, width), BF),
            pltpu.VMEM((half_edges, width), BF),
            pltpu.VMEM((width, hidden), BF),
            pltpu.VMEM((1, hidden), F32),
            pltpu.VMEM(senders.shape, jnp.int32),
            pltpu.VMEM(receivers.shape, jnp.int32),
            pltpu.VMEM((n_grid + width, hidden), BF),
            pltpu.VMEM((EDGE_BLOCK, n_grid + width), BF),
            dma((7,)),
        ],
        compiler_params=small,
        cost_estimate=pl.CostEstimate(flops=SENDER_FLOPS, transcendentals=0, bytes_accessed=1 << 22),
        name="sender_step",
    )(
        *scalars(band.reshape(1), chan.reshape(1), edge_count),
        *wide(grid_latent),
        near(grid_far),
        *wide(edge_latent),
        near(edge_far),
        *wide(w_grid, w_edge, bias.reshape(1, hidden), senders, receivers),
    )

    mesh_low, mesh_high, pre, left, right = lax.optimization_barrier((mesh_low, mesh_high, pre, left, right))
    mesh_near = (mesh_low, mesh_own, mesh_high)
    mesh_far = [near(swap(mesh_low)), *wide(mesh_own_far), near(swap(mesh_high))]
    wire, cots, seg_grid, rim_low, rim_mid, rim_high = pl.pallas_call(
        edge_kernel,
        out_shape=(
            pltpu.HBM((MEMBERS, 2 * ROWS + TAIL, LANES), BF),
            pltpu.VMEM((n_edges, hidden), BF),
            pltpu.VMEM((n_grid, hidden), BF),
            pltpu.HBM((2 * piece, hidden), BF),
            pltpu.VMEM((2 * piece, hidden), F32),
            pltpu.HBM((2 * piece, hidden), BF),
        ),
        in_specs=[anywhere] * 7 + [vmem, anywhere, vmem, anywhere, anywhere, vmem, vmem, vmem],
        out_specs=(anywhere, vmem, vmem, anywhere, vmem, anywhere),
        scratch_shapes=[
            pltpu.VMEM((n_grid, width), BF),
            pltpu.VMEM((n_edges, width), BF),
            pltpu.VMEM((pad_mesh, width), BF),
            pltpu.VMEM((pad_mesh, width), BF),
            pltpu.VMEM((pad_mesh, 3 * hidden), BF),
            pltpu.VMEM((n_edges, 2 * hidden), BF),
            pltpu.VMEM((pad_mesh, 2 * hidden), F32),
            pltpu.VMEM((width, hidden), BF),
            pltpu.VMEM((hidden, width), BF),
            pltpu.VMEM((MEMBERS, 2 * ROWS + 16, LANES), BF),
            pltpu.VMEM((2 * piece, hidden), BF),
            pltpu.VMEM((2 * piece, hidden), BF),
            dma((12,)),
            dma((n_edges // UNIT,)),
            dma((6,)),
        ],
        compiler_params=large,
        cost_estimate=pl.CostEstimate(flops=EDGE_FLOPS, transcendentals=1 << 20, bytes_accessed=1 << 23),
        name="edge_step",
    )(
        *wide(grid_latent, grid_far, edge_latent, edge_far, *mesh_near),
        *mesh_far,
        *wide(w_mesh, w_out),
        near(pre),
        near(left),
        near(right),
    )

    cot_own, cot_far = (cots[:half_edges], cots[half_edges:])
    from_low = pair_swap(rim_low, 0)
    from_high = pair_swap(rim_high, 1)
    arrived = lax.all_to_all(wire, GROUP, 0, 0, tiled=True)
    edge_term = dot_t(cot_far, w_edge).astype(BF)
    grid_term = dot_t(seg_grid[half_grid:], w_grid).astype(BF)
    edge_back = swap(edge_term)
    grid_back = swap(grid_term)
    total = arrived.astype(F32).sum(axis=0).astype(BF)
    grad_edge = (dot_t(cot_own, w_edge) + edge_back.astype(F32)).astype(BF)
    grad_grid = (dot_t(seg_grid[:half_grid], w_grid) + grid_back.astype(F32)).astype(BF)
    total, from_low, from_high, grad_edge, grad_grid = lax.optimization_barrier(
        (total, from_low, from_high, grad_edge, grad_grid)
    )
    total = depth_total(total)
    grad_bias = total[2 * ROWS : 2 * ROWS + 2].reshape(hidden)
    chunk = jnp.concatenate([total[:ROWS], total[ROWS : 2 * ROWS]], axis=1).astype(BF)
    spread = jnp.broadcast_to(chunk[None], (MEMBERS, ROWS, hidden))
    everyone = lax.all_to_all(spread, GROUP, 0, 0, tiled=True)

    seg_mesh = (rim_mid + from_low.astype(F32) + from_high.astype(F32)).astype(BF)
    seg_mesh, _ = lax.optimization_barrier((seg_mesh, chunk))
    mesh_back = swap(dot_t(seg_mesh[piece:], w_mesh).astype(BF))
    grad_mesh = (dot_t(seg_mesh[:piece], w_mesh) + mesh_back.astype(F32)).astype(BF)

    def rows_of(start, stop):
        return everyone[start:stop].astype(F32).reshape(-1, hidden)

    q = MEMBERS // 4
    return (
        grad_grid,
        grad_edge,
        grad_mesh,
        rows_of(0, q),
        rows_of(q, 2 * q),
        rows_of(2 * q, 3 * q),
        grad_bias,
        jnp.concatenate([rows_of(3 * q, 3 * q + q // 2), rows_of(3 * q + q // 2, 4 * q)], axis=1),
    )


def solution(mesh):
    bands, chans = (mesh.shape["band"], mesh.shape["chan"])
    side = 4
    inner = Mesh(np.asarray(mesh.devices).reshape(bands // (2 * side**2), 2, side, side, chans), (*BAND, "chan"))
    every = P((*BAND, "chan"), None)
    return jax.shard_map(
        body,
        mesh=inner,
        in_specs=(
            every,
            every,
            every,
            every,
            P(None, "chan"),
            P(None, "chan"),
            P(None, "chan"),
            P("chan"),
            P("chan", None),
            P(BAND),
            P(BAND),
            P(BAND),
        ),
        out_specs=(
            every,
            every,
            every,
            P(None, "chan"),
            P(None, "chan"),
            P(None, "chan"),
            P("chan"),
            P("chan", None),
        ),
        check_vma=False,
    )
```

```python
import functools

import jax
import jax.numpy as jnp
import numpy as np
from jax import lax
from jax.experimental import pallas as pl
from jax.experimental.pallas import tpu as pltpu
from jax.sharding import Mesh, PartitionSpec as P


BF = jnp.bfloat16
F32 = jnp.float32
BAND = ("zh", "zl", "y", "x")
GROUP = ("zl", "y", "x")
LANES = 128
EDGE_BLOCK = 768
UNIT = 384
TAIL = 8
ROWS = 64
MEMBERS = 32
SENDER_FLOPS = 4 * 10**9
EDGE_FLOPS = 9 * 10**9


def dot(a, b):
    return jnp.dot(a, b, preferred_element_type=F32)


def dot_t(a, b):
    return lax.dot_general(a, b, (((1,), (1,)), ((), ())), preferred_element_type=F32)


def dot_rows(a, b):
    return lax.dot_general(a, b, (((0,), (0,)), ((), ())), preferred_element_type=F32)


def one_hot(column, offset):
    place = lax.broadcasted_iota(jnp.int32, column.shape, column.ndim - 1)
    return jnp.where(column == place + offset, 1.0, 0.0).astype(BF)


def one_hot_rows(row, offset):
    place = lax.broadcasted_iota(jnp.int32, row.shape, 0)
    return jnp.where(row == place + offset, 1.0, 0.0).astype(BF)


def local_senders(row, where, half_grid):
    at = row - where[0] * (2 * half_grid) - where[1] * half_grid
    return jnp.where(at < 0, at + 2 * half_grid, at)


def local_receivers(row, slot, where, piece):
    at = row - (where[0] - 1) * (2 * piece)
    owner = jnp.where(at >= 2 * piece, 1, 0) + jnp.where(at >= 4 * piece, 1, 0)
    within = at - owner * (2 * piece)
    half = jnp.where(within >= piece, 1, 0)
    flip = jnp.where(half == where[1], 0, 1)
    place = jnp.where(where[0] % 2 == 0, 2 - owner, owner)
    near = (flip * 3 + place) * piece + within - half * piece
    return jnp.where(slot < where[2], near, -1)


def index_row(group, groups, where):
    at = group + where[1] * (groups // 2)
    return jnp.where(at >= groups, at - groups, at)


def copies(pairs, sems):
    return [pltpu.make_async_copy(src, dst, sems.at[k]) for k, (src, dst) in enumerate(pairs)]


def sender_kernel(
    piece,
    band,
    chan,
    count,
    grid_own,
    grid_far,
    edge_own,
    edge_far,
    w_grid,
    w_edge,
    bias_in,
    send_in,
    recv_in,
    pre,
    left_mesh,
    right,
    grid,
    edge,
    weights,
    bias_row,
    senders,
    receivers,
    table,
    left,
    in_sems,
):
    where = (band[0], chan[0], count[0])
    half_edges = edge_own.shape[0]
    half_grid = grid_own.shape[0]
    n_grid = 2 * half_grid
    block = left.shape[0]
    fetches = copies(
        (
            (w_grid, weights),
            (grid_own, grid),
            (send_in, senders),
            (recv_in, receivers),
            (w_edge, table.at[n_grid:]),
            (bias_in, bias_row),
            (edge_own, edge),
        ),
        in_sems,
    )
    for f in fetches:
        f.start()
    fetches[0].wait()
    table[half_grid:n_grid] = dot(grid_far[...], weights[...]).astype(BF)
    fetches[1].wait()
    table[0:half_grid] = dot(grid[...], weights[...]).astype(BF)
    for f in fetches[2:]:
        f.wait()
    groups = 2 * half_edges // LANES
    per = block // LANES
    units = block // UNIT
    near = half_edges // UNIT

    def step(i, carry):
        rows = pl.ds(pl.multiple_of(i * block, block), block)
        for h in range(units):
            at = i * units + h
            mine = slice(h * UNIT, (h + 1) * UNIT)

            @pl.when(at < near)
            def _():
                left[mine, n_grid:] = edge[pl.ds(pl.multiple_of(at * UNIT, UNIT), UNIT), :]

            @pl.when(at >= near)
            def _():
                left[mine, n_grid:] = edge_far[pl.ds(pl.multiple_of((at - near) * UNIT, UNIT), UNIT), :]

        for c in range(per):
            at = index_row(i * per + c, groups, where)
            mine = pl.ds(pl.multiple_of(i * block + c * LANES, LANES), LANES)
            row = local_senders(senders[pl.ds(at, 1), :], where, half_grid)
            row = jnp.broadcast_to(row, (LANES, LANES))
            column = row.T
            for k in range(n_grid // LANES):
                left[c * LANES : (c + 1) * LANES, k * LANES : (k + 1) * LANES] = one_hot(column, k * LANES)
                right[k * LANES : (k + 1) * LANES, mine] = one_hot_rows(row, k * LANES)
            slot = at * LANES + lax.broadcasted_iota(jnp.int32, (1, LANES), 1)
            row = local_receivers(receivers[pl.ds(at, 1), :], slot, where, piece)
            row = jnp.broadcast_to(row, (LANES, LANES))
            column = row.T
            for k in range(left_mesh.shape[1] // LANES):
                left_mesh[mine, k * LANES : (k + 1) * LANES] = one_hot(column, k * LANES)
                at_row = n_grid + k * LANES
                right[at_row : at_row + LANES, mine] = one_hot_rows(row, k * LANES)
        pre[rows, :] = dot(left[...], table[...]) + bias_row[...]
        return carry

    lax.fori_loop(0, 2 * half_edges // block, step, 0)


def edge_kernel(
    grid_own,
    grid_far,
    edge_own,
    edge_far,
    m0,
    m1,
    m2,
    m3,
    m4,
    m5,
    w_mesh_in,
    w_out_in,
    pre_part,
    left,
    right,
    wire_out,
    cots,
    seg_grid,
    rim_low,
    rim_mid,
    rim_high,
    grid,
    edge,
    lat,
    cot,
    table,
    both,
    sums,
    w_mesh,
    w_out,
    wire,
    low_v,
    high_v,
    in_sems,
    edge_sems,
    out_sems,
):
    half_edges = edge_own.shape[0]
    half_grid = grid_own.shape[0]
    n_grid = 2 * half_grid
    piece = m0.shape[1]
    n_mesh = 6 * piece
    pad_mesh = lat.shape[0]
    block = EDGE_BLOCK
    hidden = w_mesh.shape[1]
    near = half_edges // UNIT
    apart = ((0, m0), (1, m1), (2, m2), (4, m4))
    lats = [(m.at[0], lat.at[k * piece : (k + 1) * piece]) for k, m in apart]
    cot_pairs = [(m.at[1], cot.at[k * piece : (k + 1) * piece]) for k, m in apart]
    grids = [(grid_own, grid.at[0:half_grid]), (grid_far, grid.at[half_grid:])]
    small = [(w_mesh_in, w_mesh), (w_out_in, w_out)]
    fetches = copies(small + lats + cot_pairs + grids, in_sems)
    edges = [
        (source.at[k * UNIT : (k + 1) * UNIT], edge.at[(k + off) * UNIT : (k + off + 1) * UNIT])
        for source, off in ((edge_own, 0), (edge_far, near))
        for k in range(near)
    ]
    for f in fetches[0:10] + copies(edges, edge_sems) + fetches[10:]:
        f.start()
    for k, m in ((3, m3), (5, m5)):
        lat[k * piece : (k + 1) * piece] = m[0]
        cot[k * piece : (k + 1) * piece] = m[1]
    if pad_mesh > n_mesh:
        lat[n_mesh:] = jnp.zeros((pad_mesh - n_mesh, lat.shape[1]), BF)
        cot[n_mesh:] = jnp.zeros((pad_mesh - n_mesh, cot.shape[1]), BF)
    for f in fetches[0:10]:
        f.wait()
    table[:, 0:hidden] = dot(lat[...], w_mesh[...]).astype(BF)
    cot_terms = dot_t(cot[...], w_out[...])
    high = cot_terms.astype(BF)
    table[:, hidden : 2 * hidden] = high
    table[:, 2 * hidden :] = (cot_terms - high.astype(F32)).astype(BF)

    def step(i, carry):
        rows = pl.ds(pl.multiple_of(i * block, block), block)
        got = dot(left[rows, :], table[...])
        pre = pre_part[rows, :] + got[:, 0:hidden]
        hidden_cot = got[:, hidden : 2 * hidden] + got[:, 2 * hidden :]
        sig = jax.nn.sigmoid(pre)
        act = (pre * sig).astype(BF)
        pre_cot = (hidden_cot * sig * (1.0 + pre * (1.0 - sig))).astype(BF)
        cots[rows, :] = pre_cot
        both[rows, 0:hidden] = pre_cot
        both[rows, hidden:] = act
        return carry

    lax.fori_loop(0, 2 * half_edges // block, step, 0)

    grid_tile = n_grid // 3
    mesh_tile = pad_mesh // 2

    def sum_grid(t, carry):
        at = pl.ds(pl.multiple_of(t * grid_tile, grid_tile), grid_tile)
        seg_grid[at, :] = dot(right[at, :], both[:, 0:hidden]).astype(BF)
        return carry

    def sum_mesh(t, carry):
        at = pl.multiple_of(t * mesh_tile, mesh_tile)
        sums[pl.ds(at, mesh_tile), :] = dot(right[pl.ds(n_grid + at, mesh_tile), :], both[...])
        return carry

    lax.fori_loop(0, 2, sum_mesh, 0)
    lax.fori_loop(0, 3, sum_grid, 0)
    for ref, o, kind in ((low_v, 0, BF), (rim_mid, 1, F32), (high_v, 2, BF)):
        for h in range(2):
            start = (3 * h + o) * piece
            ref[h * piece : (h + 1) * piece] = sums[start : start + piece, 0:hidden].astype(kind)
    rows = ROWS
    per_grad = w_mesh.shape[0] // rows
    parts = [slice(k * per_grad, (k + 1) * per_grad) for k in range(4)]
    stores = copies(
        [(low_v, rim_low), (high_v, rim_high)] + [(wire.at[p, 0 : 2 * ROWS + TAIL], wire_out.at[p]) for p in parts],
        out_sems,
    )
    for f in stores[0:2]:
        f.start()
    for f in fetches[10:] + copies(edges, edge_sems):
        f.wait()
    sub = lax.broadcasted_iota(jnp.int32, (16, LANES), 0)
    bias_total = dot(jnp.ones((16, 2 * half_edges), BF), both[:, 0:hidden])
    tail = jnp.where(sub == 0, bias_total[:, :LANES], jnp.where(sub == 1, bias_total[:, LANES:], 0.0)).astype(BF)
    for k in range(wire.shape[0]):
        wire[k, 2 * rows :, :] = tail

    def put_all(at, g):
        for k in range(g.shape[0] // rows):
            value = g[k * rows : (k + 1) * rows]
            wire[at + k, 0:rows, :] = value[:, :LANES].astype(BF)
            wire[at + k, rows : 2 * rows, :] = value[:, LANES:].astype(BF)

    put_all(parts[2].start, dot_rows(edge[...], both[:, 0:hidden]))
    stores[4].start()
    put_all(parts[0].start, dot_rows(grid[...], seg_grid[...]))
    stores[2].start()
    put_all(parts[1].start, dot_rows(lat[...], sums[:, 0:hidden].astype(BF)))
    stores[3].start()
    g = dot_rows(sums[:, hidden:].astype(BF), cot[...])
    put_all(parts[3].start, g[:, 0:hidden])
    put_all(parts[3].start + per_grad // 2, g[:, hidden:])
    stores[5].start()
    for f in stores:
        f.wait()


def swap(x):
    return lax.ppermute(x, "chan", [(0, 1), (1, 0)])


def pair_swap(x, first):
    n = lax.axis_size(BAND)
    pairs = [(i, i + 1) for i in range(first, n - 1, 2)]
    return lax.ppermute(x, BAND, pairs + [(j, i) for i, j in pairs])


def depth_total(mine):
    depth = lax.axis_size("zh")
    step = 1
    while True:
        mask = depth - 1 if 2 * step == depth else step
        other = lax.ppermute(mine, "zh", [(i, i ^ mask) for i in range(depth)])
        total = mine.astype(F32) + other.astype(F32)
        step *= 2
        if step == depth:
            return total
        mine = total.astype(BF)


def body(
    grid_latent,
    edge_latent,
    mesh_latent,
    mesh_cotangent,
    w_grid,
    w_mesh,
    w_edge,
    bias,
    w_out,
    senders,
    receivers,
    edge_count,
):
    band = lax.axis_index(BAND)
    chan = lax.axis_index("chan")
    half_grid = grid_latent.shape[0]
    half_edges = edge_latent.shape[0]
    piece, width = mesh_latent.shape
    hidden = w_grid.shape[1]
    n_grid = 2 * half_grid
    pad_mesh = -(-6 * piece // LANES) * LANES

    mesh_own = jnp.stack([mesh_latent, mesh_cotangent])
    mesh_low = pair_swap(mesh_own, 0)
    mesh_high = pair_swap(mesh_own, 1)
    edge_far = swap(edge_latent)
    grid_far = swap(grid_latent)
    mesh_own_far = swap(mesh_own)

    senders = senders.reshape(-1, LANES)
    receivers = receivers.reshape(-1, LANES)
    vmem = pl.BlockSpec(memory_space=pltpu.VMEM)
    smem = pl.BlockSpec(memory_space=pltpu.SMEM)
    small, large = [pltpu.CompilerParams(vmem_limit_bytes=n * 2**20) for n in (12, 26)]

    def near(x):
        return pltpu.with_memory_space_constraint(x, pltpu.VMEM)

    def wide(*arrays):
        return [pltpu.with_memory_space_constraint(x, pltpu.HBM) for x in arrays]

    def scalars(*arrays):
        return [pltpu.with_memory_space_constraint(x, pltpu.SMEM) for x in arrays]

    anywhere = pl.BlockSpec(memory_space=pl.ANY)
    dma = pltpu.SemaphoreType.DMA
    n_edges = 2 * half_edges
    pre, left, right = pl.pallas_call(
        functools.partial(sender_kernel, piece),
        out_shape=(
            pltpu.VMEM((n_edges, hidden), F32),
            pltpu.VMEM((n_edges, pad_mesh), BF),
            pltpu.VMEM((n_grid + pad_mesh, n_edges), BF),
        ),
        in_specs=[smem] * 3 + [anywhere, vmem] * 2 + [anywhere] * 5,
        out_specs=(vmem,) * 3,
        scratch_shapes=[
            pltpu.VMEM((half_grid, width), BF),
            pltpu.VMEM((half_edges, width), BF),
            pltpu.VMEM((width, hidden), BF),
            pltpu.VMEM((1, hidden), F32),
            pltpu.VMEM(senders.shape, jnp.int32),
            pltpu.VMEM(receivers.shape, jnp.int32),
            pltpu.VMEM((n_grid + width, hidden), BF),
            pltpu.VMEM((EDGE_BLOCK, n_grid + width), BF),
            dma((7,)),
        ],
        compiler_params=small,
        cost_estimate=pl.CostEstimate(flops=SENDER_FLOPS, transcendentals=0, bytes_accessed=1 << 22),
        name="sender_step",
    )(
        *scalars(band.reshape(1), chan.reshape(1), edge_count),
        *wide(grid_latent),
        near(grid_far),
        *wide(edge_latent),
        near(edge_far),
        *wide(w_grid, w_edge, bias.reshape(1, hidden), senders, receivers),
    )

    mesh_low, mesh_high, pre, left, right = lax.optimization_barrier((mesh_low, mesh_high, pre, left, right))
    mesh_near = (mesh_low, mesh_own, mesh_high)
    mesh_far = [near(swap(mesh_low)), *wide(mesh_own_far), near(swap(mesh_high))]
    wire, cots, seg_grid, rim_low, rim_mid, rim_high = pl.pallas_call(
        edge_kernel,
        out_shape=(
            pltpu.HBM((MEMBERS, 2 * ROWS + TAIL, LANES), BF),
            pltpu.VMEM((n_edges, hidden), BF),
            pltpu.VMEM((n_grid, hidden), BF),
            pltpu.HBM((2 * piece, hidden), BF),
            pltpu.VMEM((2 * piece, hidden), F32),
            pltpu.HBM((2 * piece, hidden), BF),
        ),
        in_specs=[anywhere] * 7 + [vmem, anywhere, vmem, anywhere, anywhere, vmem, vmem, vmem],
        out_specs=(anywhere, vmem, vmem, anywhere, vmem, anywhere),
        scratch_shapes=[
            pltpu.VMEM((n_grid, width), BF),
            pltpu.VMEM((n_edges, width), BF),
            pltpu.VMEM((pad_mesh, width), BF),
            pltpu.VMEM((pad_mesh, width), BF),
            pltpu.VMEM((pad_mesh, 3 * hidden), BF),
            pltpu.VMEM((n_edges, 2 * hidden), BF),
            pltpu.VMEM((pad_mesh, 2 * hidden), F32),
            pltpu.VMEM((width, hidden), BF),
            pltpu.VMEM((hidden, width), BF),
            pltpu.VMEM((MEMBERS, 2 * ROWS + 16, LANES), BF),
            pltpu.VMEM((2 * piece, hidden), BF),
            pltpu.VMEM((2 * piece, hidden), BF),
            dma((12,)),
            dma((n_edges // UNIT,)),
            dma((6,)),
        ],
        compiler_params=large,
        cost_estimate=pl.CostEstimate(flops=EDGE_FLOPS, transcendentals=1 << 20, bytes_accessed=1 << 23),
        name="edge_step",
    )(
        *wide(grid_latent, grid_far, edge_latent, edge_far, *mesh_near),
        *mesh_far,
        *wide(w_mesh, w_out),
        near(pre),
        near(left),
        near(right),
    )

    cot_own, cot_far = (cots[:half_edges], cots[half_edges:])
    arrived = lax.all_to_all(wire, GROUP, 0, 0, tiled=True)
    edge_term = dot_t(cot_far, w_edge).astype(BF)
    grid_term = dot_t(seg_grid[half_grid:], w_grid).astype(BF)
    edge_back = swap(edge_term)
    grid_back = swap(grid_term)
    total = arrived.astype(F32).sum(axis=0).astype(BF)
    grad_edge = (dot_t(cot_own, w_edge) + edge_back.astype(F32)).astype(BF)
    grad_grid = (dot_t(seg_grid[:half_grid], w_grid) + grid_back.astype(F32)).astype(BF)
    total, rim_low, rim_high, grad_edge, grad_grid = lax.optimization_barrier(
        (total, rim_low, rim_high, grad_edge, grad_grid)
    )
    from_low = pair_swap(rim_low, 0)
    from_high = pair_swap(rim_high, 1)
    total = depth_total(total)
    grad_bias = total[2 * ROWS : 2 * ROWS + 2].reshape(hidden)
    chunk = jnp.concatenate([total[:ROWS], total[ROWS : 2 * ROWS]], axis=1).astype(BF)
    spread = jnp.broadcast_to(chunk[None], (MEMBERS, ROWS, hidden))
    everyone = lax.all_to_all(spread, GROUP, 0, 0, tiled=True)

    seg_mesh = (rim_mid + from_low.astype(F32) + from_high.astype(F32)).astype(BF)
    seg_mesh, _ = lax.optimization_barrier((seg_mesh, chunk))
    mesh_back = swap(dot_t(seg_mesh[piece:], w_mesh).astype(BF))
    grad_mesh = (dot_t(seg_mesh[:piece], w_mesh) + mesh_back.astype(F32)).astype(BF)

    def rows_of(start, stop):
        return everyone[start:stop].astype(F32).reshape(-1, hidden)

    q = MEMBERS // 4
    return (
        grad_grid,
        grad_edge,
        grad_mesh,
        rows_of(0, q),
        rows_of(q, 2 * q),
        rows_of(2 * q, 3 * q),
        grad_bias,
        jnp.concatenate([rows_of(3 * q, 3 * q + q // 2), rows_of(3 * q + q // 2, 4 * q)], axis=1),
    )


def solution(mesh):
    bands, chans = (mesh.shape["band"], mesh.shape["chan"])
    side = 4
    inner = Mesh(np.asarray(mesh.devices).reshape(bands // (2 * side**2), 2, side, side, chans), (*BAND, "chan"))
    every = P((*BAND, "chan"), None)
    return jax.shard_map(
        body,
        mesh=inner,
        in_specs=(
            every,
            every,
            every,
            every,
            P(None, "chan"),
            P(None, "chan"),
            P(None, "chan"),
            P("chan"),
            P("chan", None),
            P(BAND),
            P(BAND),
            P(BAND),
        ),
        out_specs=(
            every,
            every,
            every,
            P(None, "chan"),
            P(None, "chan"),
            P(None, "chan"),
            P("chan"),
            P("chan", None),
        ),
        check_vma=False,
    )
```
